32 devices in a mesh: dp: 2 (over x), fsdp: 4 (over y, core), tensor: 4 (over z).
Axes of the slice: x: 2, y: 2, z: 4, core: 2. Of those that a mesh axis runs over, the one named last changes fastest.
Arguments:
- hidden: bfloat16 [4096, 2048], P(('dp', 'fsdp'), 'tensor'), may hold values from -8 to 8
- norm_gain: bfloat16 [2048], P('tensor'), may hold values from 0.099609375 to 1.8984375
- head_weight: bfloat16 [2048, 32128], P('fsdp', 'tensor'), may hold values from -1 to 1
- token_ids: int32 [8, 512], P(('dp', 'fsdp')), may hold values from 0 to 32127
- lengths: int32 [8], P(('dp', 'fsdp')), may hold values from 128 to 512
- old_logp: float32 [8, 512], P(('dp', 'fsdp')), may hold values from -12.5 to -9.5
- advantages: float32 [8, 512], P(('dp', 'fsdp')), may hold values from -4 to 4
- rollout_logp: float32 [8, 512], P(('dp', 'fsdp'), 'tensor'), may hold values from -16 to -1
- rollout_row: int32 [8], P(('dp', 'fsdp')), may hold values from 0 to 7, each once
Outputs:
- new_logp: float32 [8, 512], P(('dp', 'fsdp'))
- token_loss: float32 [8, 512], P(('dp', 'fsdp'))
- summary: float32 [3], replicated
The draws below stay inside these ranges and needn't reach their ends.
Inputs may be any that keep to these rules, and one draw needn't show every extreme that they name: `rollout_row`: every row 0 to 7 is named once.
All inputs are finite; a program needn't handle non-finite values.
Results may differ from the reference program's by a relative error of at most 0.0005.
The reference program's roundings to bfloat16 on the way (of `normed`) count: a program that leaves them out, or rounds other values in their place, can miss the bound.
Values may be sent and summed in bfloat16 or wider, within the bound.
A program may use at most 128 MiB of HBM per device.

```python
import math
import jax
import jax.numpy as jnp
import numpy as np
from jax import lax

D = 2048
VOCAB = 32128
LEN = 512
RESP = 8
TOKENS = 4096


def draw_hidden(key, part):
    samples = jax.random.normal(jax.random.fold_in(key, 21), (TOKENS, D), jnp.float32)
    return jnp.clip(samples, -8.0, 8.0).astype(jnp.bfloat16)


def draw_head_weight(key, part):
    weights = jax.random.normal(jax.random.fold_in(key, 31), (D, VOCAB), jnp.float32) / math.sqrt(D)
    return jnp.clip(weights, -1.0, 1.0).astype(jnp.bfloat16)


def draw_lengths(key, part):
    row_index = jnp.arange(RESP, dtype=jnp.int32)
    shortest = LEN // 4
    rising = shortest + row_index * (LEN - shortest) // max(RESP - 1, 1)
    jitter = jax.random.randint(jax.random.fold_in(key, 41), (RESP,), 0, LEN // 8 + 1)
    values = jnp.clip(rising - jitter, shortest, LEN)
    values = jnp.where(row_index == RESP - 1, LEN, values)
    values = jnp.where(row_index == 0, shortest, values)
    return values.astype(jnp.int32)


def draw_rollout_logp(key, part):
    center = -math.log(VOCAB)
    row_offset = jax.random.uniform(jax.random.fold_in(key, 51), (RESP, 1), jnp.float32, -2.0, 2.0)
    token_jitter = jax.random.uniform(jax.random.fold_in(key, 52), (RESP, LEN), jnp.float32, -1.0, 1.0)
    return jnp.clip(center + row_offset + token_jitter, -16.0, -1.0)


def with_ends(array, rng, smallest, largest):
    longest = array.shape.index(max(array.shape))
    spots = []
    for shift in (0, 1):
        where = [jax.random.randint(jax.random.fold_in(rng, axis), (), 0, length) for axis, length in enumerate(array.shape)]
        where[longest] = (where[longest] + shift) % array.shape[longest]
        spots.append(tuple(where))
    return array.at[spots[0]].set(smallest).at[spots[1]].set(largest)


def block_levels(key, dims, cuts, low, high):
    loudness, own = 1.0, jax.random.fold_in(key, 6)
    for dim, parts in cuts:
        draws = jnp.exp(jax.random.uniform(jax.random.fold_in(own, dim), (parts,), jnp.float32, low / len(cuts), high / len(cuts)))
        loudness = loudness * jnp.repeat(draws, dims[dim] // parts).reshape([-1 if axis == dim else 1 for axis in range(len(dims))])
    return loudness


def cumulative_ranks(amount, slope):
    portions = [(1 << 20) // math.isqrt(rank ** slope) + 1 for rank in range(1, amount + 1)]
    deviation = 1 + sum(portions) // (1 << 30)
    return np.cumsum(np.array([max(1, weight // deviation) for weight in portions]))


def ranked_ids(stream_key, extent, amount, skew):
    listing = cumulative_ranks(amount, skew)
    lot = jax.random.randint(jax.random.fold_in(stream_key, 1), extent, 0, int(listing[amount - 1]))
    standing = jnp.searchsorted(jnp.asarray(listing, jnp.int32), lot, side="right")
    return jax.random.permutation(jax.random.fold_in(stream_key, 2), amount)[standing].astype(jnp.int32)


def noise(own_key, extent, deviation, most, cuts=(), kind=jnp.bfloat16):
    drawn = jax.random.normal(own_key, extent, jnp.float32) * deviation
    if len(cuts) > 0:
        drawn = block_levels(own_key, extent, cuts, -0.22, 0.18) * drawn
    return jnp.clip(drawn, min=-most, max=most).astype(kind)


def setup_inputs(seed: int = 0) -> dict:
    splits = jax.random.split(jax.random.key(seed), 10)
    hidden = draw_hidden(jax.random.fold_in(splits[9], 71), 0)
    norm_gain = jnp.clip(1.0 + 0.18 * jax.random.normal(splits[1], (D,), jnp.float32), 0.099609375, 1.8984375).astype(jnp.bfloat16)
    head_weight = draw_head_weight(jax.random.fold_in(splits[9], 71), 0)
    token_ids = with_ends(ranked_ids(splits[3], (RESP, LEN), VOCAB, 2), jax.random.fold_in(splits[3], 3), 0, VOCAB - 1).astype(jnp.int32)
    lengths = draw_lengths(jax.random.fold_in(splits[9], 71), 0)
    old_logp = jnp.clip(-12.5 + 3.0 * jax.random.uniform(splits[5], (RESP, LEN), jnp.float32) ** block_levels(splits[5], (RESP, LEN), ((0, 8),), -0.2, 0.2), -12.5, -9.5)
    advantages = noise(splits[6], (RESP, LEN), 1.0, 4.0, ((0, 8),), jnp.float32)
    rollout_logp = draw_rollout_logp(jax.random.fold_in(splits[9], 71), 0)
    rollout_row = jax.random.permutation(splits[8], RESP).astype(jnp.int32)
    return {"hidden": hidden, "norm_gain": norm_gain, "head_weight": head_weight, "token_ids": token_ids, "lengths": lengths, "old_logp": old_logp, "advantages": advantages, "rollout_logp": rollout_logp, "rollout_row": rollout_row}


clip_eps = 0.2
kl_coef = 0.2
log_limit = 10.0
norm_eps = 1e-06

def token_terms(new_logp, old_logp, advantages, ref_logp, live_mask, prob_square):
    shift = new_logp - old_logp
    prob_ratio = jnp.exp(jnp.clip(shift, -log_limit, log_limit))
    clipped = jnp.clip(prob_ratio, 1.0 - clip_eps, 1.0 + clip_eps)
    plain_term = prob_ratio * advantages
    bounded_term = clipped * advantages
    surrogate = jnp.minimum(plain_term, bounded_term)
    ref_gap = ref_logp - new_logp
    gap_clip = jnp.clip(ref_gap, -log_limit, log_limit)
    kl_term = jnp.exp(gap_clip) - gap_clip - 1.0
    token_loss = live_mask * (kl_coef * kl_term - surrogate)
    inside_gap = (jnp.abs(ref_gap) < log_limit).astype(jnp.float32)
    inside_ratio = (jnp.abs(shift) < log_limit).astype(jnp.float32)
    active_term = (plain_term <= bounded_term).astype(jnp.float32)
    grad_coef = live_mask * (kl_coef * (1.0 - jnp.exp(gap_clip)) * inside_gap - advantages * prob_ratio * active_term * inside_ratio)
    grad_square = grad_coef * grad_coef * (prob_square - 2.0 * jnp.exp(new_logp) + 1.0)
    return (token_loss, live_mask * kl_term, grad_square)

def reference(hidden, norm_gain, head_weight, token_ids, lengths, old_logp, advantages, rollout_logp, rollout_row):
    values = hidden.astype(jnp.float32)
    inv_rms = lax.rsqrt(lax.optimization_barrier(jnp.mean(values * values, axis=1, keepdims=True)) + norm_eps)
    normed = (values * inv_rms * norm_gain.astype(jnp.float32)[None, :]).astype(jnp.bfloat16)
    blocks = normed.reshape(token_ids.shape[0], token_ids.shape[1], normed.shape[1])

    def per_response(block):
        block_rows, block_ids = block
        logits = jnp.dot(block_rows, head_weight, preferred_element_type=jnp.float32)
        row_max = lax.optimization_barrier(jnp.max(logits, axis=1))
        shifted = jnp.exp(logits - row_max[:, None])
        exp_sum = lax.optimization_barrier(jnp.sum(shifted, axis=1))
        exp_square = lax.optimization_barrier(jnp.sum(shifted * shifted, axis=1))
        picked = jnp.take_along_axis(logits, block_ids[:, None].astype(jnp.int32), axis=1)[:, 0]
        return (picked - row_max - jnp.log(exp_sum), exp_square / (exp_sum * exp_sum))
    new_logp, prob_square = lax.map(per_response, (blocks, token_ids))
    ref_logp = jnp.take(rollout_logp, rollout_row.astype(jnp.int32), axis=0)
    positions = lax.broadcasted_iota(jnp.int32, token_ids.shape, 1)
    live_mask = (positions < lengths[:, None]).astype(jnp.float32)
    token_loss, kl_part, grad_part = token_terms(new_logp, old_logp, advantages, ref_logp, live_mask, prob_square)
    live_count = jnp.sum(live_mask)
    summary = jnp.stack([jnp.sum(token_loss) / live_count, jnp.sum(kl_part) / live_count, jnp.sqrt(jnp.sum(grad_part) / live_count)])
    return (new_logp, token_loss, summary)
```

```python
import functools

import jax
import jax.numpy as jnp
from jax import lax
from jax.experimental import pallas as pl
from jax.experimental.pallas import tpu as pltpu
from jax.sharding import PartitionSpec as P

MESH = pl.DeviceIdType.MESH
clip_eps = 0.2
kl_coef = 0.2
log_limit = 10.0
norm_eps = 1e-06
LANES = 128
LOW = -1e30
UNITS_PER_TICK = 4
LEAD = 3
Z_RING = 4
Y_RING = 8


def token_terms(new_logp, old_logp, advantages, ref_logp, live_mask, prob_square):
    shift = new_logp - old_logp
    prob_ratio = jnp.exp(jnp.clip(shift, -log_limit, log_limit))
    clipped = jnp.clip(prob_ratio, 1.0 - clip_eps, 1.0 + clip_eps)
    plain_term = prob_ratio * advantages
    bounded_term = clipped * advantages
    surrogate = jnp.minimum(plain_term, bounded_term)
    ref_gap = ref_logp - new_logp
    gap_clip = jnp.clip(ref_gap, -log_limit, log_limit)
    gap_exp = jnp.exp(gap_clip)
    kl_term = gap_exp - gap_clip - 1.0
    token_loss = live_mask * (kl_coef * kl_term - surrogate)
    gap_part = jnp.where(jnp.abs(ref_gap) < log_limit, kl_coef * (1.0 - gap_exp), 0.0)
    active = (plain_term <= bounded_term) & (jnp.abs(shift) < log_limit)
    grad_coef = live_mask * (gap_part - jnp.where(active, plain_term, 0.0))
    grad_square = grad_coef * grad_coef * (prob_square - 2.0 * jnp.exp(new_logp) + 1.0)
    return (token_loss, live_mask * kl_term, grad_square)


class Config:
    def __init__(self, mesh, tok, dz, kr, vt):
        self.dp, self.fs, self.tz = (mesh.shape[a] for a in ("dp", "fsdp", "tensor"))
        self.groups = self.fs // 2
        self.tok, self.dz, self.kr, self.vt = tok, dz, kr, vt
        self.dim = dz * self.tz
        self.resp = self.dp * self.fs
        tiles = -(-vt // LANES)
        self.half_tiles = -(-tiles // (self.groups * self.dp))
        self.half_cols = self.half_tiles * LANES
        self.block_cols = self.half_cols * self.dp
        self.steps = 16 if self.groups * self.tz <= 32 else 8
        self.rows = tok // self.steps
        self.chunks = max(j for j in range(1, self.steps + 1) if self.half_tiles % j == 0)
        self.chunk = self.half_cols // self.chunks
        self.pairs = 4
        self.per_pair = self.steps // self.pairs
        self.pair_rows = tok // self.pairs
        self.width = self.groups * self.pair_rows
        self.span = 2 if self.chunks % 2 == 0 else 1
        self.blocks = self.chunks // self.span
        self.unit_cols = self.span * self.chunk
        self.gain_rows = dz // LANES
        self.plan()

    def plan(self):
        Q, Z, J = self.steps, self.tz, self.chunks
        self.ticks = Q + Z - 1
        tau = 1.0 / (Z - 1)
        start = [0.0]
        for i in range(self.ticks - 1):
            start.append(start[-1] + tau * sum(0 <= i - s < Q for s in range(Z - 1)))

        def tick_at(t):
            return min(range(len(start)), key=lambda i: abs(start[i] - t))

        last = self.ticks - 1
        rate = 13.35 / J
        self.y_tick = [tick_at(0.85 + rate * (j + 1)) for j in range(J)]
        self.x_tick = [min(last, max(t + 1, tick_at(start[t] + 1.25))) for t in self.y_tick]
        self.r_tick = [min(last, t + 1) for t in self.x_tick]
        done, self.order, self.counts = set(), [], []
        for i in range(self.ticks + 1):
            n = 0
            for k in range(self.blocks):
                for p in range(self.pairs):
                    final = p == self.pairs - 1
                    tokens = i > last if final else (p + 1) * self.per_pair + Z - 2 <= i
                    if (p, k) in done or not tokens or self.r_tick[(k + 1) * self.span - 1] > i:
                        continue
                    if n < UNITS_PER_TICK or i >= last:
                        done.add((p, k))
                        self.order.append((p, k))
                        n += 1
            self.counts.append(len(self.order))


def lookup(index, table):
    value = jnp.int32(table[0])
    for t in range(1, len(table)):
        if table[t] != table[t - 1]:
            value = value + jnp.where(index >= t, table[t] - table[t - 1], 0)
    return value


def due(i, ticks):
    count = jnp.int32(0)
    for t in ticks:
        count = count + jnp.where(i >= t, 1, 0)
    return count


def kernel(
    c,
    hid, gain_in, w_any, id_any, roll_any, old_any, adv_any, len_in, row_in,
    out,
    id_buf, roll_buf, old_buf, adv_buf,
    x_buf, n_buf, w_stage, w_full, packs, ids_all, rel, m_buf, l_buf, q_buf, p_buf,
    row_buf, roll, s_out, s_all, t_out, t_in,
    small_sem, x_sem, stage_sem, own_sem, tok_recv, y_recv, y_send, right_send, left_send,
    wy_send, wy_recv, wx_send, wx_recv, core_send, core_recv,
    ids_send, ids_recv, pack_right, pack_left, pack_recv, roll_send, roll_recv,
    st_send, st_recv, tot_send, tot_recv,
):
    G, Z, DP, F, Q, J = c.groups, c.tz, c.dp, c.fs, c.steps, c.chunks
    x = lax.axis_index("dp")
    f = lax.axis_index("fsdp")
    z = lax.axis_index("tensor")
    g, core = f // 2, f % 2
    partner = (x, g * 2 + (1 - core), z)
    me_resp = x * F + f
    right_dev = (x, f, jnp.minimum(z + 1, Z - 1))
    left_dev = (x, f, jnp.maximum(z - 1, 0))
    has_right, has_left = z + 1 < Z, z >= 1

    def dev_g(gi):
        return (x, gi * 2 + core, z)

    def dev_x(xi):
        return (xi, f, z)

    def group(d):
        return lax.rem(g + d, G)

    def remote(src, dst, ss, rs, dev):
        return pltpu.make_async_remote_copy(
            src_ref=src, dst_ref=dst, send_sem=ss, recv_sem=rs, device_id=dev, device_id_type=MESH
        )

    def arrive(dst, rs):
        remote(dst, dst, rs, rs, partner).wait_recv()

    def begin(copy):
        copy.start()

    def sent(copy):
        copy.wait_send()

    barrier = pltpu.get_barrier_semaphore()
    peers = [dev_g(group(d)) for d in range(1, G)] + [partner]
    peers += [dev_x(lax.rem(x + d, DP)) for d in range(1, DP)]
    for dev in peers:
        pl.semaphore_signal(barrier, inc=1, device_id=dev, device_id_type=MESH)
    for cond, dev in ((has_right, right_dev), (has_left, left_dev)):
        @pl.when(cond)
        def _(dev=dev):
            pl.semaphore_signal(barrier, inc=1, device_id=dev, device_id_type=MESH)

    zcols = pl.ds(pl.multiple_of(z * c.dz, c.dz), c.dz)
    fcols = pl.ds(pl.multiple_of(f * c.kr, c.kr), c.kr)
    load_x = pltpu.make_async_copy(hid, x_buf.at[g, :, zcols], x_sem)
    load_x.start()
    smalls = [
        pltpu.make_async_copy(a, b, small_sem.at[n])
        for n, (a, b) in enumerate(
            ((id_any, id_buf), (roll_any, roll_buf), (old_any, old_buf), (adv_any, adv_buf))
        )
    ]
    for copy in smalls:
        copy.start()

    def weight_loads(act):
        for own in (False, True):
            for gi in range(G):
                for h in range(DP):
                    start = gi * c.block_cols + h * c.half_cols
                    size = max(0, min(c.half_cols, c.vt - start))
                    src = w_any.at[pl.ds(start, size), :]

                    @pl.when(gi == g if own else (gi != g) & (x == h))
                    def _():
                        if own:
                            dst, sem = w_full.at[pl.ds(h * c.half_cols, size), fcols], own_sem.at[h]
                        else:
                            dst, sem = w_stage.at[gi, pl.ds(0, size), :], stage_sem.at[gi]
                        act(own, size, lambda: pltpu.make_async_copy(src, dst, sem), gi, h)

    def load_begin(own, size, copy, gi, h):
        if size:
            copy().start()
        if size < c.half_cols:
            zeros = jnp.zeros((c.half_cols - size, c.kr), w_full.dtype)
            if own:
                w_full[pl.ds(h * c.half_cols + size, c.half_cols - size), fcols] = zeros
            else:
                w_stage[gi, size:, :] = zeros

    weight_loads(load_begin)

    gain = gain_in[...].astype(jnp.float32).reshape(1, c.dz)
    for r in range(c.gain_rows):
        packs[z, r : r + 1, :] = gain[:, r * LANES : (r + 1) * LANES]
    part = roll_buf.shape[1]
    smalls[1].wait()
    tail = [roll_buf[...]] if part == LANES else [roll_buf[...], jnp.zeros((1, LANES - part), jnp.float32)]
    packs[z, c.gain_rows :, :] = jnp.broadcast_to(
        jnp.concatenate(tail, axis=1), (8 - c.gain_rows, LANES)
    )
    m_buf[...] = jnp.full(m_buf.shape, LOW, jnp.float32)
    for ref in (l_buf, q_buf, p_buf):
        ref[...] = jnp.zeros(ref.shape, jnp.float32)
    smalls[0].wait()
    ids_all[g] = id_buf[...]
    load_x.wait()

    neighbours = jnp.where(has_right, 1, 0) + jnp.where(has_left, 1, 0)
    pl.semaphore_wait(barrier, len(peers) + neighbours)

    def piece(gi, q, zi):
        return x_buf.at[
            gi, pl.ds(pl.multiple_of(q * c.rows, c.rows), c.rows), pl.ds(pl.multiple_of(zi * c.dz, c.dz), c.dz)
        ]

    def w_block(fi, h, j):
        return w_full.at[
            pl.ds(pl.multiple_of(h * c.half_cols + j * c.chunk, c.chunk), c.chunk),
            pl.ds(pl.multiple_of(fi * c.kr, c.kr), c.kr),
        ]

    def y_tokens(q, act):
        for d in range(1, G):
            act(remote(piece(g, q, z), piece(g, q, z), y_send.at[d - 1], y_recv.at[G - d - 1, lax.rem(q, Y_RING)], dev_g(group(d))))

    def y_weights(j, act):
        for d in range(1, G):
            gi = group(d)
            src = w_stage.at[gi, pl.ds(pl.multiple_of(j * c.chunk, c.chunk), c.chunk), :]
            act(remote(src, w_block(f, x, j), wy_send.at[d - 1], wy_recv.at[G - d - 1, j], dev_g(gi)))

    def hop_ends(s):
        return ((z - s >= 0, jnp.maximum(z - s, 0), has_right, right_dev, right_send, pack_right),
                (z + s < Z, jnp.minimum(z + s, Z - 1), has_left, left_dev, left_send, pack_left))

    def hop_wait(q, s, d):
        gi = group(d)
        if s == 0:
            arrive(piece(gi, q, z), y_recv.at[d - 1, lax.rem(q, Y_RING)])
            return
        for ok, zi, _, _, _, _ in hop_ends(s):
            @pl.when(ok)
            def _():
                arrive(piece(gi, q, zi), tok_recv.at[gi, lax.rem(q, Z_RING), zi])

    def hop_send(q, s, gi, act):
        for ok, zi, has, dev, sem, _ in hop_ends(s):
            @pl.when(ok & has)
            def _():
                act(remote(piece(gi, q, zi), piece(gi, q, zi), sem.at[gi, zi], tok_recv.at[gi, lax.rem(q, Z_RING), zi], dev))

    def pack_wait(s):
        for ok, zi, _, _, _, _ in hop_ends(s):
            @pl.when(ok)
            def _():
                arrive(packs.at[zi], pack_recv.at[zi])

    def pack_hop(s, act):
        for ok, zi, has, dev, _, sem in hop_ends(s):
            @pl.when(ok & has)
            def _():
                act(remote(packs.at[zi], packs.at[zi], sem.at[zi], pack_recv.at[zi], dev))

    def core_pass(src, fi, h, j, act):
        gi = fi // 2
        act(remote(src, w_block(fi, h, j), core_send.at[gi, h], core_recv.at[j], partner))

    def x_weights(d, fi, j, act):
        for dx in range(1, DP):
            act(remote(w_block(fi, x, j), w_block(fi, x, j), wx_send.at[d - 1, dx - 1],
                       wx_recv.at[d - 1, DP - dx - 1, j], dev_x(lax.rem(x + dx, DP))))

    def ids_move(act):
        for d in range(1, G):
            act(remote(id_buf, ids_all.at[g], ids_send.at[d - 1], ids_recv.at[G - d - 1], dev_g(group(d))))

    def roll_move(act):
        for dx in range(DP):
            for df in range(F):
                if dx or df:
                    act(remote(row_buf, roll.at[me_resp], roll_send, roll_recv,
                               (lax.rem(x + dx, DP), lax.rem(f + df, F), z)))

    def stats_move(p, late, act):
        for s in range(Z - 1, -1, -1):
            for d in range(G):
                if s or d:
                    gi, zi = group(d), lax.rem(z + s, Z)
                    act(remote(s_out.at[p, gi], s_all.at[p * (G * Z) + g * Z + z], st_send.at[late], st_recv.at[late],
                               (x, gi * 2 + core, zi)))

    def normalize(q):
        rows = pl.ds(pl.multiple_of(q * c.rows, c.rows), c.rows)
        for gi in range(G):
            values = x_buf[gi, rows, :].astype(jnp.float32)
            inv = lax.rsqrt(jnp.sum(values * values, axis=1, keepdims=True) / c.dim + norm_eps)
            to = (q // c.per_pair) * c.width + gi * c.pair_rows + (q % c.per_pair) * c.rows
            there = pl.ds(pl.multiple_of(to, c.rows), c.rows)
            for zi in range(Z):
                for r in range(c.gain_rows):
                    here = slice(zi * c.dz + r * LANES, zi * c.dz + (r + 1) * LANES)
                    scaled = values[:, here] * inv * packs[zi, r : r + 1, :]
                    n_buf[there, here] = scaled.astype(jnp.bfloat16)

    def unit(p, k):
        tokens = n_buf[pl.ds(pl.multiple_of(p * c.width, c.width), c.width), :]
        index = lax.broadcasted_iota(jnp.int32, (c.unit_cols // 8, 8, 1), 0) * 8 + lax.broadcasted_iota(
            jnp.int32, (c.unit_cols // 8, 8, 1), 1
        )
        for h in range(DP):
            off = h * c.half_cols + k * c.unit_cols
            cols = pl.ds(pl.multiple_of(off, c.chunk), c.unit_cols)
            logits = lax.dot_general(
                w_full[cols, :], tokens, (((1,), (1,)), ((), ())), preferred_element_type=jnp.float32
            ).reshape(c.unit_cols // 8, 8, c.width)
            valid = c.vt - g * c.block_cols - off
            place = rel[p] - off
            p_buf[p] = p_buf[p] + jnp.sum(jnp.where(index == place[None], logits, 0.0), axis=0)
            logits = jnp.where(index < valid, logits, LOW)
            before = m_buf[p]
            top = jnp.maximum(before, jnp.max(logits, axis=0))
            scale = jnp.exp(before - top)
            e = jnp.exp(logits - top[None])
            m_buf[p] = top
            l_buf[p] = l_buf[p] * scale + jnp.sum(e, axis=0)
            q_buf[p] = q_buf[p] * (scale * scale) + jnp.sum(e * e, axis=0)

    def collect(p):
        m_p = m_buf[p]
        top = jnp.max(m_p, axis=0, keepdims=True)
        scale = jnp.exp(m_p - top)
        total = jnp.sum(l_buf[p] * scale, axis=0, keepdims=True)
        square = jnp.sum(q_buf[p] * (scale * scale), axis=0, keepdims=True)
        picked = jnp.sum(p_buf[p], axis=0, keepdims=True)
        values = jnp.concatenate([top, total, square, picked, jnp.zeros((4, c.width), jnp.float32)], axis=0)
        for gi in range(G):
            s_out[p, gi] = values[:, gi * c.pair_rows : (gi + 1) * c.pair_rows]

    def collect_send(p, late):
        collect(p)
        stats_move(p, late, begin)
        s_all[p * (G * Z) + g * Z + z] = s_out[p, g]

    pack_hop(0, begin)
    for q in range(min(2, Q)):
        y_tokens(q, begin)
    ids_move(begin)

    def wait_loads(stage):
        def act(own, size, copy, gi, h):
            if size and own != stage:
                copy().wait()
        weight_loads(act)

    def tick(i, seen):
        y_first, x_first, r_first, u_first = seen
        @pl.when(i == 0)
        def _():
            wait_loads(True)
            for q in range(2, LEAD):
                y_tokens(q, begin)
            for j in range(min(LEAD - 1, J)):
                y_weights(j, begin)

        @pl.when(i + LEAD < Q)
        def _():
            y_tokens(i + LEAD, begin)

        @pl.when(i + LEAD - 1 < J)
        def _():
            y_weights(i + LEAD - 1, begin)

        for s in range(Z):
            q = i - s

            @pl.when((q >= 0) & (q < Q))
            def _(s=s, q=q):
                if s:
                    @pl.when(q == 0)
                    def _():
                        pack_wait(s)
                        if s < Z - 1:
                            pack_hop(s, begin)
                for d in range(G):
                    if s or d:
                        hop_wait(q, s, d)
                    if s < Z - 1:
                        hop_send(q, s, group(d), begin)

        @pl.when(i == 1)
        def _():
            wait_loads(False)

        @pl.when((i >= 1) & (i - 1 < J))
        def _():
            for h in range(DP):
                core_pass(w_block(f, h, i - 1), f, h, i - 1, begin)

        y_end = due(i, c.y_tick)

        @pl.loop(y_first, y_end)
        def _(j):
            for d in range(1, G):
                gi = group(d)
                fi = gi * 2 + core
                arrive(w_block(fi, x, j), wy_recv.at[d - 1, j])
                x_weights(d, fi, j, begin)
                core_pass(w_block(fi, x, j), fi, x, j, begin)

        x_end = due(i, c.x_tick)

        @pl.loop(x_first, x_end)
        def _(j):
            for d in range(1, G):
                gi = group(d)
                fi = gi * 2 + core
                for dx in range(1, DP):
                    xi = lax.rem(x + dx, DP)
                    arrive(w_block(fi, xi, j), wx_recv.at[d - 1, dx - 1, j])
                    core_pass(w_block(fi, xi, j), fi, xi, j, begin)

        q = i - (Z - 1)

        @pl.when((q >= 0) & (q < Q))
        def _():
            normalize(q)

        @pl.when(i == Z)
        def _():
            for zi in range(Z):
                row_buf[:, zi * part : (zi + 1) * part] = packs[zi, c.gain_rows : c.gain_rows + 1, :part]
            for d in range(1, G):
                arrive(ids_all.at[group(d)], ids_recv.at[d - 1])
            base = z * c.vt + g * c.block_cols
            for p in range(c.pairs):
                for gi in range(G):
                    ids = ids_all[gi, :, p * c.pair_rows : (p + 1) * c.pair_rows]
                    rel[p, :, gi * c.pair_rows : (gi + 1) * c.pair_rows] = jnp.broadcast_to(
                        ids - base, (8, c.pair_rows)
                    )

        r_end = due(i, c.r_tick)

        @pl.loop(r_first, r_end)
        def _(j):
            arrive(w_full.at[pl.ds(0, G * DP * c.kr * c.chunk // c.dim), :], core_recv.at[j])

        @pl.when(i == c.ticks)
        def _():
            roll_move(begin)
            pl.loop(0, c.pairs - 1)(lambda p: collect_send(p, 0))

        u_end = lookup(i, c.counts)

        @pl.loop(u_first, u_end)
        def _(u):
            unit(lookup(u, [p for p, _ in c.order]), lookup(u, [k for _, k in c.order]))

        return y_end, x_end, r_end, u_end

    lax.fori_loop(0, c.ticks + 1, tick, (jnp.int32(0),) * 4)
    collect_send(c.pairs - 1, 1)

    for copy in smalls[2:]:
        copy.wait()
    def done(ref, sem):
        remote(ref, ref, sem, sem, partner).wait_send()

    def features(gi, zi):
        return x_buf.at[gi, :, pl.ds(pl.multiple_of(zi * c.dz, c.dz), c.dz)]

    stage = w_stage.at[0]
    for d in range(1, G):
        done(features(g, z), y_send.at[d - 1])
        done(stage, wy_send.at[d - 1])
        for dx in range(1, DP):
            done(stage, wx_send.at[d - 1, dx - 1])
    for gi in range(G):
        for h in range(DP):
            done(stage, core_send.at[gi, h])
        for zi in range(Z):
            for cond, sem in (((zi <= z) & has_right, right_send), ((zi >= z) & has_left, left_send)):
                @pl.when(cond)
                def _():
                    done(features(gi, zi), sem.at[gi, zi])

    for s in range(Z - 1):
        pack_hop(s, sent)
    ids_move(sent)
    roll[me_resp] = row_buf[...]
    arrive(roll.at[pl.ds(0, c.resp - 1)], roll_recv)
    ref = jnp.zeros((1, c.tok), jnp.float32)
    row = row_in[...]
    for r in range(c.resp):
        ref = ref + jnp.where(row == r, roll[r], 0.0)
    position = lax.broadcasted_iota(jnp.int32, (1, c.tok), 1)
    live = jnp.where(position < len_in[...], 1.0, 0.0)
    old, adv = old_buf[...], adv_buf[...]

    tiles = G * Z - 1
    arrive(s_all.at[pl.ds(0, (c.pairs - 1) * tiles)], st_recv.at[0])
    arrive(s_all.at[pl.ds(0, tiles)], st_recv.at[1])
    every = [(gi, zi) for gi in range(G) for zi in range(Z)]

    def stat(gi, zi, k):
        return jnp.concatenate([s_all[p * (G * Z) + gi * Z + zi, k : k + 1, :] for p in range(c.pairs)], axis=1)

    top = stat(0, 0, 0)
    for gi, zi in every[1:]:
        top = jnp.maximum(top, stat(gi, zi, 0))
    total = square = picked = jnp.zeros((1, c.tok), jnp.float32)
    for gi, zi in every:
        scale = jnp.exp(stat(gi, zi, 0) - top)
        total = total + stat(gi, zi, 1) * scale
        square = square + stat(gi, zi, 2) * (scale * scale)
        picked = picked + stat(gi, zi, 3)
    new_logp = picked - top - jnp.log(total)
    prob_square = square / (total * total)
    token_loss, kl_part, grad_part = token_terms(new_logp, old, adv, ref, live, prob_square)
    sums = [jnp.sum(v, axis=1, keepdims=True) for v in (live, token_loss, kl_part, grad_part)]
    t_out[...] = jnp.concatenate(
        [jnp.broadcast_to(v, (1, LANES)) for v in sums] + [jnp.zeros((4, LANES), jnp.float32)], axis=0
    )

    def totals_move(act):
        for dx in range(DP):
            for df in range(F):
                if dx or df:
                    act(remote(t_out, t_in.at[me_resp], tot_send, tot_recv,
                               (lax.rem(x + dx, DP), lax.rem(f + df, F), z)))

    totals_move(begin)
    t_in[me_resp] = t_out[...]
    out[0:1, :] = new_logp
    out[1:2, :] = token_loss
    out[3:8, :] = jnp.zeros((5, c.tok), jnp.float32)
    done(roll.at[pl.ds(0, c.resp - 1)], roll_send)
    done(s_all.at[pl.ds(0, (c.pairs - 1) * tiles)], st_send.at[0])
    done(s_all.at[pl.ds(0, tiles)], st_send.at[1])
    arrive(t_in.at[pl.ds(0, c.resp - 1)], tot_recv)
    totals = sum(t_in[r] for r in range(c.resp))
    count = totals[0:1]
    lane = lax.broadcasted_iota(jnp.int32, (1, LANES), 1)
    means = jnp.where(lane == 0, totals[1:2] / count,
                      jnp.where(lane == 1, totals[2:3] / count, jnp.sqrt(totals[3:4] / count)))
    out[2:3, :] = jnp.concatenate([means] * (c.tok // LANES), axis=1)
    done(t_in.at[pl.ds(0, c.resp - 1)], tot_send)


def split(src, logp, loss, summary):
    logp[...] = src[0:1, :]
    loss[...] = src[1:2, :]
    summary[...] = src[2:3, 0:3].reshape(3)


def shards(c_of, hidden, norm_gain, head_weight, token_ids, lengths, old_logp, advantages, rollout_logp, rollout_row):
    c = c_of(hidden.shape[0], hidden.shape[1], head_weight.shape[0], head_weight.shape[1])
    G, Z, DP, F, Q, J = c.groups, c.tz, c.dp, c.fs, c.steps, c.chunks
    vmem = pl.BlockSpec(memory_space=pltpu.VMEM)
    hbm = pl.BlockSpec(memory_space=pl.ANY)
    dma = lambda *shape: pltpu.SemaphoreType.DMA(shape)
    one_sem = pltpu.SemaphoreType.DMA
    f32, i32, b16 = jnp.float32, jnp.int32, jnp.bfloat16
    one = lambda dtype, lead=(): pltpu.VMEM((*lead, 1, c.tok), dtype)
    lanes = lambda dtype: pltpu.VMEM((c.pairs, 8, c.width), dtype)
    out = pl.pallas_call(
        functools.partial(kernel, c),
        out_shape=jax.ShapeDtypeStruct((8, c.tok), f32),
        in_specs=[hbm, vmem, hbm, hbm, hbm, hbm, hbm, vmem, vmem],
        out_specs=vmem,
        scratch_shapes=[
            one(i32), pltpu.VMEM(rollout_logp.shape, f32), one(f32), one(f32),
            pltpu.VMEM((G, c.tok, c.dim), b16),
            pltpu.VMEM((c.pairs * c.width, c.dim), b16),
            pltpu.VMEM((G, c.half_cols, c.kr), b16),
            pltpu.VMEM((c.block_cols, c.dim), b16),
            pltpu.VMEM((Z, 8, LANES), f32),
            one(i32, (G,)),
            lanes(i32), lanes(f32), lanes(f32), lanes(f32), lanes(f32),
            one(f32), one(f32, (c.resp,)),
            pltpu.VMEM((c.pairs, G, 8, c.pair_rows), f32),
            pltpu.VMEM((c.pairs * G * Z, 8, c.pair_rows), f32),
            pltpu.VMEM((8, LANES), f32),
            pltpu.VMEM((c.resp, 8, LANES), f32),
            dma(4), one_sem, dma(G), dma(DP), dma(G, Z_RING, Z), dma(G - 1, Y_RING), dma(G - 1), dma(G, Z), dma(G, Z),
            dma(G - 1), dma(G - 1, J), dma(G - 1, DP - 1), dma(G - 1, DP - 1, J), dma(G, DP), dma(J),
            dma(G - 1), dma(G - 1), dma(Z), dma(Z), dma(Z), one_sem, one_sem,
            dma(2), dma(2), one_sem, one_sem,
        ],
        compiler_params=pltpu.CompilerParams(
            collective_id=0, has_side_effects=True, vmem_limit_bytes=64 * 1024 * 1024 - 65536
        ),
    )(hidden, norm_gain, head_weight.T, token_ids, rollout_logp, old_logp, advantages,
      lengths.reshape(1, 1), rollout_row.reshape(1, 1))
    row = lambda n: jax.ShapeDtypeStruct((1, c.tok), f32)
    return pl.pallas_call(
        split,
        out_shape=(row(0), row(1), jax.ShapeDtypeStruct((3,), f32)),
        in_specs=[vmem],
        out_specs=(vmem, vmem, vmem),
    )(out)


def solution(mesh):
    rows = ("dp", "fsdp")
    in_specs = (
        P(rows, "tensor"), P("tensor"), P("fsdp", "tensor"), P(rows, None), P(rows),
        P(rows, None), P(rows, None), P(rows, "tensor"), P(rows),
    )
    out_specs = (P(rows, None), P(rows, None), P())
    return jax.shard_map(
        functools.partial(shards, functools.partial(Config, mesh)),
        mesh=mesh, in_specs=in_specs, out_specs=out_specs, check_vma=False,
    )
```

```python
import functools

import jax
import jax.numpy as jnp
from jax import lax
from jax.experimental import pallas as pl
from jax.experimental.pallas import tpu as pltpu
from jax.sharding import PartitionSpec as P

MESH = pl.DeviceIdType.MESH
clip_eps = 0.2
kl_coef = 0.2
log_limit = 10.0
norm_eps = 1e-06
LANES = 128
LOW = -1e30
UNITS_PER_TICK = 2
LEAD = 3
Z_RING = 4
TICK, W_STEP, W_AHEAD, Y_LAG, X_LAG, SLACK = 4.25, 2.8, 3, 3.2, 2.4, 1.0


def token_terms(new_logp, old_logp, advantages, ref_logp, live_mask, prob_square):
    shift = new_logp - old_logp
    prob_ratio = jnp.exp(jnp.clip(shift, -log_limit, log_limit))
    clipped = jnp.clip(prob_ratio, 1.0 - clip_eps, 1.0 + clip_eps)
    plain_term = prob_ratio * advantages
    bounded_term = clipped * advantages
    surrogate = jnp.minimum(plain_term, bounded_term)
    ref_gap = ref_logp - new_logp
    gap_clip = jnp.clip(ref_gap, -log_limit, log_limit)
    gap_exp = jnp.exp(gap_clip)
    kl_term = gap_exp - gap_clip - 1.0
    token_loss = live_mask * (kl_coef * kl_term - surrogate)
    gap_part = jnp.where(jnp.abs(ref_gap) < log_limit, kl_coef * (1.0 - gap_exp), 0.0)
    active = (plain_term <= bounded_term) & (jnp.abs(shift) < log_limit)
    grad_coef = live_mask * (gap_part - jnp.where(active, plain_term, 0.0))
    grad_square = grad_coef * grad_coef * (prob_square - 2.0 * jnp.exp(new_logp) + 1.0)
    return (token_loss, live_mask * kl_term, grad_square)


class Config:
    def __init__(self, mesh, tok, dz, kr, vt):
        self.dp, self.fs, self.tz = (mesh.shape[a] for a in ("dp", "fsdp", "tensor"))
        self.groups = self.fs // 2
        self.tok, self.dz, self.kr, self.vt = tok, dz, kr, vt
        self.dim = dz * self.tz
        self.resp = self.dp * self.fs
        tiles = -(-vt // LANES)
        self.half_tiles = -(-tiles // (self.groups * self.dp))
        self.half_cols = self.half_tiles * LANES
        self.block_cols = self.half_cols * self.dp
        self.rows = 64
        self.group_steps = tok // self.rows
        self.steps = self.groups * self.group_steps
        self.chunks = max(j for j in range(1, 17) if self.half_tiles % j == 0)
        self.chunk = self.half_cols // self.chunks
        self.width = 256
        self.per_pair = self.width // self.rows
        self.group_pairs = tok // self.width
        self.pairs = self.groups * self.group_pairs
        self.span = next(n for n in (4, 2, 1) if self.chunks % n == 0)
        self.blocks = self.chunks // self.span
        self.unit_cols = self.span * self.chunk
        self.gain_rows = dz // LANES
        self.plan()

    def plan(self):
        N, Z, J, T = self.steps, self.tz, self.chunks, self.group_steps
        self.ticks = N + Z - 1
        last = self.ticks - 1
        at = [TICK * (n - 0.3) if n < N + 1 else TICK * (N + 0.7) + (n - N - 1) * TICK / 2 for n in range(self.ticks)]

        def tick_at(t, low):
            return min([n for n in range(low, last) if at[n] >= t - SLACK], default=last)

        alone = max(0, T - LEAD)
        step = W_STEP * N / J
        self.w_tick, self.y_tick, self.x_tick, self.r_tick = [], [], [], []
        x_free = 0.0
        for j in range(J):
            early = W_AHEAD + TICK / step * alone
            n = max(0, -(-(j + 1 - W_AHEAD) * step // TICK)) if j < early else alone + (j + 1 - early) * N / J
            self.w_tick.append(min(last, int(n)))
            t = Y_LAG + step * (j + 1) + (max(0, j + 1 - early + W_AHEAD) * (TICK - step) if j + 1 > early - W_AHEAD else 0)
            y = tick_at(t, self.w_tick[-1] + 1)
            x_free = max(x_free, at[y]) + step
            x = tick_at(x_free + X_LAG, y + 1)
            r = min(last, x + 1)
            self.y_tick.append(y)
            self.x_tick.append(x)
            self.r_tick.append(r)
        done, self.order, self.counts = set(), [], []
        for i in range(self.ticks):
            n = 0
            for k in range(self.blocks):
                for p in range(self.pairs - 1):
                    if (p, k) in done or (p + 1) * self.per_pair + Z - 2 > i or self.r_tick[(k + 1) * self.span - 1] > i:
                        continue
                    if n < UNITS_PER_TICK or i >= last:
                        done.add((p, k))
                        self.order.append((p, k))
                        n += 1
            self.counts.append(len(self.order))


def lookup(index, table):
    value = jnp.int32(table[0])
    for t in range(1, len(table)):
        if table[t] != table[t - 1]:
            value = value + jnp.where(index >= t, table[t] - table[t - 1], 0)
    return value


def due(i, ticks):
    count = jnp.int32(0)
    for t in ticks:
        count = count + jnp.where(i >= t, 1, 0)
    return count


def kernel(
    c,
    hid, gain_in, w_any, id_any, roll_any, old_any, adv_any, len_in, row_in,
    out,
    id_buf, roll_buf, old_buf, adv_buf,
    x_buf, n_buf, w_stage, w_full, packs, ids_all, rel, m_buf, l_buf, q_buf, p_buf,
    row_buf, roll, s_out, s_all, t_out, t_in,
    small_sem, x_sem, stage_sem, own_sem, tok_recv, y_recv, y_send, right_send, left_send,
    wy_send, wy_recv, wx_send, wx_recv, core_send, core_recv,
    ids_send, ids_recv, pack_right, pack_left, pack_recv, roll_send, roll_recv,
    st_send, st_recv, tot_send, tot_recv,
):
    G, Z, DP, F, N, T, J = c.groups, c.tz, c.dp, c.fs, c.steps, c.group_steps, c.chunks
    x = lax.axis_index("dp")
    f = lax.axis_index("fsdp")
    z = lax.axis_index("tensor")
    g, core = f // 2, f % 2
    partner = (x, g * 2 + (1 - core), z)
    me_resp = x * F + f
    right_dev = (x, f, jnp.minimum(z + 1, Z - 1))
    left_dev = (x, f, jnp.maximum(z - 1, 0))
    has_right, has_left = z + 1 < Z, z >= 1

    def dev_g(gi):
        return (x, gi * 2 + core, z)

    def dev_x(xi):
        return (xi, f, z)

    def group(d):
        return lax.rem(g + d, G)

    def remote(src, dst, ss, rs, dev):
        return pltpu.make_async_remote_copy(
            src_ref=src, dst_ref=dst, send_sem=ss, recv_sem=rs, device_id=dev, device_id_type=MESH
        )

    def arrive(dst, rs):
        remote(dst, dst, rs, rs, partner).wait_recv()

    def begin(copy):
        copy.start()

    def sent(copy):
        copy.wait_send()

    barrier = pltpu.get_barrier_semaphore()
    peers = [dev_g(group(d)) for d in range(1, G)] + [partner]
    peers += [dev_x(lax.rem(x + d, DP)) for d in range(1, DP)]
    for dev in peers:
        pl.semaphore_signal(barrier, inc=1, device_id=dev, device_id_type=MESH)
    for cond, dev in ((has_right, right_dev), (has_left, left_dev)):
        @pl.when(cond)
        def _(dev=dev):
            pl.semaphore_signal(barrier, inc=1, device_id=dev, device_id_type=MESH)

    zcols = pl.ds(pl.multiple_of(z * c.dz, c.dz), c.dz)
    fcols = pl.ds(pl.multiple_of(f * c.kr, c.kr), c.kr)
    load_x = pltpu.make_async_copy(hid, x_buf.at[g, :, zcols], x_sem)
    load_x.start()
    smalls = [
        pltpu.make_async_copy(a, b, small_sem.at[n])
        for n, (a, b) in enumerate(
            ((id_any, id_buf), (roll_any, roll_buf), (old_any, old_buf), (adv_any, adv_buf))
        )
    ]
    for copy in smalls:
        copy.start()

    def weight_loads(act):
        for own in (False, True):
            for gi in range(G):
                for h in range(DP):
                    start = gi * c.block_cols + h * c.half_cols
                    size = max(0, min(c.half_cols, c.vt - start))
                    src = w_any.at[pl.ds(start, size), :]

                    @pl.when(gi == g if own else (gi != g) & (x == h))
                    def _():
                        if own:
                            dst, sem = w_full.at[pl.ds(h * c.half_cols, size), fcols], own_sem.at[h]
                        else:
                            dst, sem = w_stage.at[gi, pl.ds(0, size), :], stage_sem.at[gi]
                        act(own, size, lambda: pltpu.make_async_copy(src, dst, sem), gi, h)

    def load_begin(own, size, copy, gi, h):
        if size:
            copy().start()
        if size < c.half_cols:
            zeros = jnp.zeros((c.half_cols - size, c.kr), w_full.dtype)
            if own:
                w_full[pl.ds(h * c.half_cols + size, c.half_cols - size), fcols] = zeros
            else:
                w_stage[gi, size:, :] = zeros

    weight_loads(load_begin)

    gain = gain_in[...].astype(jnp.float32).reshape(1, c.dz)
    for r in range(c.gain_rows):
        packs[z, r : r + 1, :] = gain[:, r * LANES : (r + 1) * LANES]
    part = roll_buf.shape[1]
    smalls[1].wait()
    tail = [roll_buf[...]] if part == LANES else [roll_buf[...], jnp.zeros((1, LANES - part), jnp.float32)]
    packs[z, c.gain_rows :, :] = jnp.broadcast_to(
        jnp.concatenate(tail, axis=1), (8 - c.gain_rows, LANES)
    )
    m_buf[...] = jnp.full(m_buf.shape, LOW, jnp.float32)
    for ref in (l_buf, q_buf, p_buf):
        ref[...] = jnp.zeros(ref.shape, jnp.float32)
    smalls[0].wait()
    ids_all[g] = id_buf[...]
    load_x.wait()

    neighbours = jnp.where(has_right, 1, 0) + jnp.where(has_left, 1, 0)
    pl.semaphore_wait(barrier, len(peers) + neighbours)

    def piece(gi, q, zi):
        return x_buf.at[
            gi, pl.ds(pl.multiple_of(q * c.rows, c.rows), c.rows), pl.ds(pl.multiple_of(zi * c.dz, c.dz), c.dz)
        ]

    def w_block(fi, h, j):
        return w_full.at[
            pl.ds(pl.multiple_of(h * c.half_cols + j * c.chunk, c.chunk), c.chunk),
            pl.ds(pl.multiple_of(fi * c.kr, c.kr), c.kr),
        ]

    def y_tokens(n, act):
        for d in range(1, G):
            q = n - (G - d) * T

            @pl.when((q >= 0) & (q < T))
            def _(d=d, q=q):
                act(remote(piece(g, q, z), piece(g, q, z), y_send.at[d - 1], y_recv.at[G - d - 1, q], dev_g(group(d))))

    def y_weights(j, act):
        for d in range(1, G):
            gi = group(d)
            src = w_stage.at[gi, pl.ds(pl.multiple_of(j * c.chunk, c.chunk), c.chunk), :]
            act(remote(src, w_block(f, x, j), wy_send.at[d - 1], wy_recv.at[G - d - 1, j], dev_g(gi)))

    def hop_ends(s):
        return ((z - s >= 0, jnp.maximum(z - s, 0), has_right, right_dev, right_send, pack_right),
                (z + s < Z, jnp.minimum(z + s, Z - 1), has_left, left_dev, left_send, pack_left))

    def locate(n):
        return group(n // T), lax.rem(n, T), lax.rem(n, Z_RING)

    def hop_wait(n, s):
        gi, q, slot = locate(n)
        if s == 0:
            @pl.when(n >= T)
            def _():
                arrive(piece(gi, q, z), y_recv.at[n // T - 1, q])
            return
        for ok, zi, _, _, _, _ in hop_ends(s):
            @pl.when(ok)
            def _():
                arrive(piece(gi, q, zi), tok_recv.at[slot, zi])

    def hop_send(n, s, act):
        gi, q, slot = locate(n)
        for ok, zi, has, dev, sem, _ in hop_ends(s):
            @pl.when(ok & has)
            def _():
                act(remote(piece(gi, q, zi), piece(gi, q, zi), sem.at[zi], tok_recv.at[slot, zi], dev))

    def pack_wait(s):
        for ok, zi, _, _, _, _ in hop_ends(s):
            @pl.when(ok)
            def _():
                arrive(packs.at[zi], pack_recv.at[zi])

    def pack_hop(s, act):
        for ok, zi, has, dev, _, sem in hop_ends(s):
            @pl.when(ok & has)
            def _():
                act(remote(packs.at[zi], packs.at[zi], sem.at[zi], pack_recv.at[zi], dev))

    def core_pass(src, fi, h, j, act):
        gi = fi // 2
        act(remote(src, w_block(fi, h, j), core_send.at[gi, h], core_recv.at[j], partner))

    def x_weights(d, fi, j, act):
        for dx in range(1, DP):
            act(remote(w_block(fi, x, j), w_block(fi, x, j), wx_send.at[d - 1, dx - 1],
                       wx_recv.at[d - 1, DP - dx - 1, j], dev_x(lax.rem(x + dx, DP))))

    def ids_move(act):
        for d in range(1, G):
            act(remote(id_buf, ids_all.at[g], ids_send.at[d - 1], ids_recv.at[G - d - 1], dev_g(group(d))))

    def roll_move(act):
        for dx in range(DP):
            for df in range(F):
                if dx or df:
                    act(remote(row_buf, roll.at[me_resp], roll_send, roll_recv,
                               (lax.rem(x + dx, DP), lax.rem(f + df, F), z)))

    def stats_move(p, late, act):
        d, half = p // c.group_pairs, lax.rem(p, c.group_pairs)
        gi = group(d)
        for s in range(Z - 1, -1, -1):
            def go(s=s):
                act(remote(s_out.at[p], s_all.at[half * (G * Z) + g * Z + z], st_send.at[late], st_recv.at[late],
                           (x, gi * 2 + core, lax.rem(z + s, Z))))
            if s:
                go()
            else:
                pl.when(d > 0)(go)

    def normalize(n):
        gi, q, _ = locate(n)
        values = x_buf[gi, pl.ds(pl.multiple_of(q * c.rows, c.rows), c.rows), :].astype(jnp.float32)
        inv = lax.rsqrt(jnp.sum(values * values, axis=1, keepdims=True) / c.dim + norm_eps)
        there = pl.ds(pl.multiple_of(n * c.rows, c.rows), c.rows)
        for zi in range(Z):
            for r in range(c.gain_rows):
                here = slice(zi * c.dz + r * LANES, zi * c.dz + (r + 1) * LANES)
                scaled = values[:, here] * inv * packs[zi, r : r + 1, :]
                n_buf[there, here] = scaled.astype(jnp.bfloat16)

    def unit(p, k):
        tokens = n_buf[pl.ds(pl.multiple_of(p * c.width, c.width), c.width), :]
        index = lax.broadcasted_iota(jnp.int32, (c.unit_cols // 8, 8, 1), 0) * 8 + lax.broadcasted_iota(
            jnp.int32, (c.unit_cols // 8, 8, 1), 1
        )
        for h in range(DP):
            off = h * c.half_cols + k * c.unit_cols
            cols = pl.ds(pl.multiple_of(off, c.chunk), c.unit_cols)
            logits = lax.dot_general(
                w_full[cols, :], tokens, (((1,), (1,)), ((), ())), preferred_element_type=jnp.float32
            ).reshape(c.unit_cols // 8, 8, c.width)
            valid = c.vt - g * c.block_cols - off
            place = rel[p] - off
            p_buf[p] = p_buf[p] + jnp.sum(jnp.where(index == place[None], logits, 0.0), axis=0)
            logits = jnp.where(index < valid, logits, LOW)
            before = m_buf[p]
            top = jnp.maximum(before, jnp.max(logits, axis=0))
            scale = jnp.exp(before - top)
            e = jnp.exp(logits - top[None])
            m_buf[p] = top
            l_buf[p] = l_buf[p] * scale + jnp.sum(e, axis=0)
            q_buf[p] = q_buf[p] * (scale * scale) + jnp.sum(e * e, axis=0)

    def collect(p):
        m_p = m_buf[p]
        top = jnp.max(m_p, axis=0, keepdims=True)
        scale = jnp.exp(m_p - top)
        total = jnp.sum(l_buf[p] * scale, axis=0, keepdims=True)
        square = jnp.sum(q_buf[p] * (scale * scale), axis=0, keepdims=True)
        picked = jnp.sum(p_buf[p], axis=0, keepdims=True)
        s_out[p] = jnp.concatenate([top, total, square, picked, jnp.zeros((4, c.width), jnp.float32)], axis=0)

    def collect_send(p, late):
        p = jnp.int32(p)
        collect(p)
        stats_move(p, late, begin)

        @pl.when(p < c.group_pairs)
        def _():
            s_all[p * (G * Z) + g * Z + z] = s_out[p]

    pack_hop(0, begin)
    ids_move(begin)

    def wait_loads(stage):
        def act(own, size, copy, gi, h):
            if size and own != stage:
                copy().wait()
        weight_loads(act)

    def tick(i, seen):
        w_first, y_first, x_first, r_first, u_first = seen

        @pl.when(i == 0)
        def _():
            wait_loads(True)

        w_end = due(i, c.w_tick)

        @pl.when(i + LEAD < N)
        def _():
            y_tokens(i + LEAD, begin)

        @pl.loop(w_first, w_end)
        def _(j):
            y_weights(j, begin)

        for s in range(Z):
            q = i - s

            @pl.when((q >= 0) & (q < N))
            def _(s=s, q=q):
                if s:
                    @pl.when(q == 0)
                    def _():
                        pack_wait(s)
                        if s < Z - 1:
                            pack_hop(s, begin)
                hop_wait(q, s)
                if s < Z - 1:
                    hop_send(q, s, begin)

        @pl.when(i == 1)
        def _():
            wait_loads(False)

        for n in range(2):
            j = 2 * (i - 1) + n

            @pl.when((j >= 0) & (j < J))
            def _(j=j):
                for h in range(DP):
                    core_pass(w_block(f, h, j), f, h, j, begin)

        y_end = due(i, c.y_tick)

        @pl.loop(y_first, y_end)
        def _(j):
            for d in range(1, G):
                gi = group(d)
                fi = gi * 2 + core
                arrive(w_block(fi, x, j), wy_recv.at[d - 1, j])
                x_weights(d, fi, j, begin)
                core_pass(w_block(fi, x, j), fi, x, j, begin)

        x_end = due(i, c.x_tick)

        @pl.loop(x_first, x_end)
        def _(j):
            for d in range(1, G):
                gi = group(d)
                fi = gi * 2 + core
                for dx in range(1, DP):
                    xi = lax.rem(x + dx, DP)
                    arrive(w_block(fi, xi, j), wx_recv.at[d - 1, dx - 1, j])
                    core_pass(w_block(fi, xi, j), fi, xi, j, begin)

        q = i - (Z - 1)

        @pl.when((q >= 0) & (q < N))
        def _():
            normalize(q)

        @pl.when(i == Z)
        def _():
            for zi in range(Z):
                row_buf[:, zi * part : (zi + 1) * part] = packs[zi, c.gain_rows : c.gain_rows + 1, :part]
            for d in range(1, G):
                arrive(ids_all.at[group(d)], ids_recv.at[d - 1])
            base = z * c.vt + g * c.block_cols
            for d in range(G):
                for half in range(c.group_pairs):
                    ids = ids_all[group(d), :, half * c.width : (half + 1) * c.width]
                    rel[d * c.group_pairs + half] = jnp.broadcast_to(ids - base, (8, c.width))

        r_end = due(i, c.r_tick)

        @pl.loop(r_first, r_end)
        def _(j):
            arrive(w_full.at[pl.ds(0, G * DP * c.kr * c.chunk // c.dim), :], core_recv.at[j])

        u_end = lookup(i, c.counts)

        @pl.loop(u_first, u_end)
        def _(u):
            unit(lookup(u, [p for p, _ in c.order]), lookup(u, [k for _, k in c.order]))

        return w_end, y_end, x_end, r_end, u_end

    lax.fori_loop(0, c.ticks, tick, (jnp.int32(0),) * 5)
    roll_move(begin)
    pl.loop(0, c.pairs - 1)(lambda p: collect_send(p, 0))
    pl.loop(0, c.blocks)(lambda k: unit(c.pairs - 1, k))
    collect_send(c.pairs - 1, 1)

    for copy in smalls[2:]:
        copy.wait()
    def done(ref, sem):
        remote(ref, ref, sem, sem, partner).wait_send()

    def features(gi, zi):
        return x_buf.at[gi, :, pl.ds(pl.multiple_of(zi * c.dz, c.dz), c.dz)]

    stage = w_stage.at[0]
    for d in range(1, G):
        done(features(g, z), y_send.at[d - 1])
        done(stage, wy_send.at[d - 1])
        for dx in range(1, DP):
            done(stage, wx_send.at[d - 1, dx - 1])
    for gi in range(G):
        for h in range(DP):
            done(stage, core_send.at[gi, h])
    for zi in range(Z):
        for cond, sem in (((zi <= z) & has_right, right_send), ((zi >= z) & has_left, left_send)):
            @pl.when(cond)
            def _():
                done(x_buf.at[:, :, pl.ds(zi * c.dz, c.dz)], sem.at[zi])

    for s in range(Z - 1):
        pack_hop(s, sent)
    ids_move(sent)
    roll[me_resp] = row_buf[...]
    arrive(roll.at[pl.ds(0, c.resp - 1)], roll_recv)
    ref = jnp.zeros((1, c.tok), jnp.float32)
    row = row_in[...]
    for r in range(c.resp):
        ref = ref + jnp.where(row == r, roll[r], 0.0)
    position = lax.broadcasted_iota(jnp.int32, (1, c.tok), 1)
    live = jnp.where(position < len_in[...], 1.0, 0.0)
    old, adv = old_buf[...], adv_buf[...]

    early = c.group_pairs * (G * Z - 1) - Z
    arrive(s_all.at[pl.ds(0, early)], st_recv.at[0])
    arrive(s_all.at[pl.ds(0, Z)], st_recv.at[1])
    every = [(gi, zi) for gi in range(G) for zi in range(Z)]

    def stat(gi, zi, k):
        return jnp.concatenate([s_all[p * (G * Z) + gi * Z + zi, k : k + 1, :] for p in range(c.group_pairs)], axis=1)

    top = stat(0, 0, 0)
    for gi, zi in every[1:]:
        top = jnp.maximum(top, stat(gi, zi, 0))
    total = square = picked = jnp.zeros((1, c.tok), jnp.float32)
    for gi, zi in every:
        scale = jnp.exp(stat(gi, zi, 0) - top)
        total = total + stat(gi, zi, 1) * scale
        square = square + stat(gi, zi, 2) * (scale * scale)
        picked = picked + stat(gi, zi, 3)
    new_logp = picked - top - jnp.log(total)
    prob_square = square / (total * total)
    token_loss, kl_part, grad_part = token_terms(new_logp, old, adv, ref, live, prob_square)
    sums = [jnp.sum(v, axis=1, keepdims=True) for v in (live, token_loss, kl_part, grad_part)]
    t_out[...] = jnp.concatenate(
        [jnp.broadcast_to(v, (1, LANES)) for v in sums] + [jnp.zeros((4, LANES), jnp.float32)], axis=0
    )

    def totals_move(act):
        for dx in range(DP):
            for df in range(F):
                if dx or df:
                    act(remote(t_out, t_in.at[me_resp], tot_send, tot_recv,
                               (lax.rem(x + dx, DP), lax.rem(f + df, F), z)))

    totals_move(begin)
    t_in[me_resp] = t_out[...]
    out[0:1, :] = new_logp
    out[1:2, :] = token_loss
    out[3:8, :] = jnp.zeros((5, c.tok), jnp.float32)
    done(roll.at[pl.ds(0, c.resp - 1)], roll_send)
    done(s_all.at[pl.ds(0, early)], st_send.at[0])
    done(s_all.at[pl.ds(0, Z)], st_send.at[1])
    arrive(t_in.at[pl.ds(0, c.resp - 1)], tot_recv)
    totals = sum(t_in[r] for r in range(c.resp))
    count = totals[0:1]
    lane = lax.broadcasted_iota(jnp.int32, (1, LANES), 1)
    means = jnp.where(lane == 0, totals[1:2] / count,
                      jnp.where(lane == 1, totals[2:3] / count, jnp.sqrt(totals[3:4] / count)))
    out[2:3, :] = jnp.concatenate([means] * (c.tok // LANES), axis=1)
    done(t_in.at[pl.ds(0, c.resp - 1)], tot_send)


def split(src, logp, loss, summary):
    logp[...] = src[0:1, :]
    loss[...] = src[1:2, :]
    summary[...] = src[2:3, 0:3].reshape(3)


def shards(c_of, hidden, norm_gain, head_weight, token_ids, lengths, old_logp, advantages, rollout_logp, rollout_row):
    c = c_of(hidden.shape[0], hidden.shape[1], head_weight.shape[0], head_weight.shape[1])
    G, Z, DP, F, T, J = c.groups, c.tz, c.dp, c.fs, c.group_steps, c.chunks
    vmem = pl.BlockSpec(memory_space=pltpu.VMEM)
    hbm = pl.BlockSpec(memory_space=pl.ANY)
    dma = lambda *shape: pltpu.SemaphoreType.DMA(shape)
    one_sem = pltpu.SemaphoreType.DMA
    f32, i32, b16 = jnp.float32, jnp.int32, jnp.bfloat16
    one = lambda dtype, lead=(): pltpu.VMEM((*lead, 1, c.tok), dtype)
    lanes = lambda dtype: pltpu.VMEM((c.pairs, 8, c.width), dtype)
    out = pl.pallas_call(
        functools.partial(kernel, c),
        out_shape=jax.ShapeDtypeStruct((8, c.tok), f32),
        in_specs=[hbm, vmem, hbm, hbm, hbm, hbm, hbm, vmem, vmem],
        out_specs=vmem,
        scratch_shapes=[
            one(i32), pltpu.VMEM(rollout_logp.shape, f32), one(f32), one(f32),
            pltpu.VMEM((G, c.tok, c.dim), b16),
            pltpu.VMEM((c.pairs * c.width, c.dim), b16),
            pltpu.VMEM((G, c.half_cols, c.kr), b16),
            pltpu.VMEM((c.block_cols, c.dim), b16),
            pltpu.VMEM((Z, 8, LANES), f32),
            one(i32, (G,)),
            lanes(i32), lanes(f32), lanes(f32), lanes(f32), lanes(f32),
            one(f32), one(f32, (c.resp,)),
            pltpu.VMEM((c.pairs, 8, c.width), f32),
            pltpu.VMEM((c.group_pairs * G * Z, 8, c.width), f32),
            pltpu.VMEM((8, LANES), f32),
            pltpu.VMEM((c.resp, 8, LANES), f32),
            dma(4), one_sem, dma(G), dma(DP), dma(Z_RING, Z), dma(G - 1, T), dma(G - 1), dma(Z), dma(Z),
            dma(G - 1), dma(G - 1, J), dma(G - 1, DP - 1), dma(G - 1, DP - 1, J), dma(G, DP), dma(J),
            dma(G - 1), dma(G - 1), dma(Z), dma(Z), dma(Z), one_sem, one_sem,
            dma(2), dma(2), one_sem, one_sem,
        ],
        compiler_params=pltpu.CompilerParams(
            collective_id=0, has_side_effects=True, vmem_limit_bytes=64 * 1024 * 1024 - 65536
        ),
    )(hidden, norm_gain, head_weight.T, token_ids, rollout_logp, old_logp, advantages,
      lengths.reshape(1, 1), rollout_row.reshape(1, 1))
    row = lambda n: jax.ShapeDtypeStruct((1, c.tok), f32)
    return pl.pallas_call(
        split,
        out_shape=(row(0), row(1), jax.ShapeDtypeStruct((3,), f32)),
        in_specs=[vmem],
        out_specs=(vmem, vmem, vmem),
    )(out)


def solution(mesh):
    rows = ("dp", "fsdp")
    in_specs = (
        P(rows, "tensor"), P("tensor"), P("fsdp", "tensor"), P(rows, None), P(rows),
        P(rows, None), P(rows, None), P(rows, "tensor"), P(rows),
    )
    out_specs = (P(rows, None), P(rows, None), P())
    return jax.shard_map(
        functools.partial(shards, functools.partial(Config, mesh)),
        mesh=mesh, in_specs=in_specs, out_specs=out_specs, check_vma=False,
    )
```

```python
import functools

import jax
import jax.numpy as jnp
from jax import lax
from jax.experimental import pallas as pl
from jax.experimental.pallas import tpu as pltpu
from jax.sharding import PartitionSpec as P

MESH = pl.DeviceIdType.MESH
clip_eps = 0.2
kl_coef = 0.2
log_limit = 10.0
norm_eps = 1e-06
LANES = 128
LOW = -1e30
UNITS_PER_TICK = 2
LEAD = 5
Z_RING = 4
TICK, FILL, W_STEP, W_AHEAD, Y_HEAD, Y_LAG, X_LAG, SLACK = 4.25, 3.8, 2.8, 12.0, 7.5, 3.5, 2.4, 1.5


def token_terms(new_logp, old_logp, advantages, ref_logp, live_mask, prob_square):
    shift = new_logp - old_logp
    prob_ratio = jnp.exp(jnp.clip(shift, -log_limit, log_limit))
    clipped = jnp.clip(prob_ratio, 1.0 - clip_eps, 1.0 + clip_eps)
    plain_term = prob_ratio * advantages
    bounded_term = clipped * advantages
    surrogate = jnp.minimum(plain_term, bounded_term)
    ref_gap = ref_logp - new_logp
    gap_clip = jnp.clip(ref_gap, -log_limit, log_limit)
    gap_exp = jnp.exp(gap_clip)
    kl_term = gap_exp - gap_clip - 1.0
    token_loss = live_mask * (kl_coef * kl_term - surrogate)
    gap_part = jnp.where(jnp.abs(ref_gap) < log_limit, kl_coef * (1.0 - gap_exp), 0.0)
    active = (plain_term <= bounded_term) & (jnp.abs(shift) < log_limit)
    grad_coef = live_mask * (gap_part - jnp.where(active, plain_term, 0.0))
    grad_square = grad_coef * grad_coef * (prob_square - 2.0 * jnp.exp(new_logp) + 1.0)
    return (token_loss, live_mask * kl_term, grad_square)


class Config:
    def __init__(self, mesh, tok, dz, kr, vt):
        self.dp, self.fs, self.tz = (mesh.shape[a] for a in ("dp", "fsdp", "tensor"))
        self.groups = self.fs // 2
        self.tok, self.dz, self.kr, self.vt = tok, dz, kr, vt
        self.dim = dz * self.tz
        self.resp = self.dp * self.fs
        tiles = -(-vt // LANES)
        self.half_tiles = -(-tiles // (self.groups * self.dp))
        self.half_cols = self.half_tiles * LANES
        self.block_cols = self.half_cols * self.dp
        self.rows = 64
        self.group_steps = tok // self.rows
        self.steps = self.groups * self.group_steps
        self.chunks = max(j for j in range(1, 17) if self.half_tiles % j == 0)
        self.chunk = self.half_cols // self.chunks
        self.width = 256
        self.per_pair = self.width // self.rows
        self.group_pairs = tok // self.width
        self.pairs = self.groups * self.group_pairs
        self.span = next(n for n in (4, 2, 1) if self.chunks % n == 0)
        self.blocks = self.chunks // self.span
        self.unit_cols = self.span * self.chunk
        self.gain_rows = dz // LANES
        self.plan()

    def plan(self):
        N, Z, J, T = self.steps, self.tz, self.chunks, self.group_steps
        self.ticks = N + Z - 1
        last = self.ticks - 1
        at = [FILL * n for n in range(Z)]
        for n in range(Z, self.ticks):
            at.append(at[-1] + TICK * sum(0 <= n - 1 - h < N for h in range(Z - 1)) / (Z - 1))

        def tick_at(t, low):
            return min([n for n in range(low, last) if at[n] >= t - SLACK], default=last)

        step = W_STEP * N / J
        alone = max(1, int((T * TICK - Y_HEAD) / step))
        self.w_tick, self.y_tick, self.x_tick, self.r_tick = [], [], [], []
        x_free = 0.0
        for j in range(J):
            begin = step * j if j < alone else step * alone + (j - alone) * TICK + TICK / 3
            self.w_tick.append(max(n for n in range(last) if n == 0 or at[n] <= begin - W_AHEAD))
            y = tick_at(begin + step + Y_LAG, self.w_tick[-1] + 1)
            x_free = max(x_free, at[y]) + step
            x = tick_at(x_free + X_LAG, y + 1)
            r = min(last, x + 1)
            self.y_tick.append(y)
            self.x_tick.append(x)
            self.r_tick.append(r)
        done, self.order, self.counts = set(), [], []
        for i in range(self.ticks):
            n = 0
            for k in range(self.blocks):
                for p in range(self.pairs - 1):
                    if (p, k) in done or (p + 1) * self.per_pair + Z - 2 > i or self.r_tick[(k + 1) * self.span - 1] > i:
                        continue
                    if n < UNITS_PER_TICK or i >= last:
                        done.add((p, k))
                        self.order.append((p, k))
                        n += 1
            self.counts.append(len(self.order))


def lookup(index, table):
    value = jnp.int32(table[0])
    for t in range(1, len(table)):
        if table[t] != table[t - 1]:
            value = value + jnp.where(index >= t, table[t] - table[t - 1], 0)
    return value


def due(i, ticks):
    count = jnp.int32(0)
    for t in ticks:
        count = count + jnp.where(i >= t, 1, 0)
    return count


def kernel(
    c,
    hid, gain_any, w_any, id_any, roll_any, old_any, adv_any, len_any, row_any,
    out,
    id_buf, roll_buf, old_buf, adv_buf, gain_in, len_in, row_in,
    x_buf, n_buf, w_stage, w_full, packs, ids_all, rel, m_buf, l_buf, q_buf, p_buf,
    row_buf, roll, s_out, s_all, t_out, t_in,
    small_sem, x_sem, stage_sem, own_sem, tok_recv, y_recv, y_send, right_send, left_send,
    wy_send, wy_recv, wx_send, wx_recv, core_send, core_recv,
    ids_send, ids_recv, pack_right, pack_left, pack_recv, roll_send, roll_recv,
    st_send, st_recv, tot_send, tot_recv,
):
    G, Z, DP, F, N, T, J = c.groups, c.tz, c.dp, c.fs, c.steps, c.group_steps, c.chunks
    x = lax.axis_index("dp")
    f = lax.axis_index("fsdp")
    z = lax.axis_index("tensor")
    g, core = f // 2, f % 2
    partner = (x, g * 2 + (1 - core), z)
    me_resp = x * F + f
    right_dev = (x, f, jnp.minimum(z + 1, Z - 1))
    left_dev = (x, f, jnp.maximum(z - 1, 0))
    has_right, has_left = z + 1 < Z, z >= 1

    def dev_g(gi):
        return (x, gi * 2 + core, z)

    def dev_x(xi):
        return (xi, f, z)

    def group(d):
        return lax.rem(g + d, G)

    def remote(src, dst, ss, rs, dev):
        return pltpu.make_async_remote_copy(
            src_ref=src, dst_ref=dst, send_sem=ss, recv_sem=rs, device_id=dev, device_id_type=MESH
        )

    def arrive(dst, rs):
        remote(dst, dst, rs, rs, partner).wait_recv()

    def begin(copy):
        copy.start()

    def sent(copy):
        copy.wait_send()

    barrier = pltpu.get_barrier_semaphore()
    peers = [dev_g(group(d)) for d in range(1, G)] + [partner]
    peers += [dev_x(lax.rem(x + d, DP)) for d in range(1, DP)]
    for dev in peers:
        pl.semaphore_signal(barrier, inc=1, device_id=dev, device_id_type=MESH)
    for cond, dev in ((has_right, right_dev), (has_left, left_dev)):
        @pl.when(cond)
        def _(dev=dev):
            pl.semaphore_signal(barrier, inc=1, device_id=dev, device_id_type=MESH)

    zcols = pl.ds(pl.multiple_of(z * c.dz, c.dz), c.dz)
    fcols = pl.ds(pl.multiple_of(f * c.kr, c.kr), c.kr)
    load_x = pltpu.make_async_copy(hid, x_buf.at[g, :, zcols], x_sem)
    load_x.start()
    smalls = [
        pltpu.make_async_copy(a, b, small_sem.at[n])
        for n, (a, b) in enumerate(
            ((id_any, id_buf), (roll_any, roll_buf), (gain_any, gain_in), (old_any, old_buf), (adv_any, adv_buf),
             (len_any, len_in), (row_any, row_in))
        )
    ]
    for copy in smalls:
        copy.start()

    def weight_loads(act):
        for own in (False, True):
            for gi in range(G):
                for h in range(DP):
                    start = gi * c.block_cols + h * c.half_cols
                    size = max(0, min(c.half_cols, c.vt - start))
                    src = w_any.at[pl.ds(start, size), :]

                    @pl.when(gi == g if own else (gi != g) & (x == h))
                    def _():
                        if own:
                            dst, sem = w_full.at[pl.ds(h * c.half_cols, size), fcols], own_sem.at[h]
                        else:
                            dst, sem = w_stage.at[gi, pl.ds(0, size), :], stage_sem.at[gi]
                        act(own, size, lambda: pltpu.make_async_copy(src, dst, sem), gi, h)

    def load_begin(own, size, copy, gi, h):
        if size:
            copy().start()
        if size < c.half_cols:
            zeros = jnp.zeros((c.half_cols - size, c.kr), w_full.dtype)
            if own:
                w_full[pl.ds(h * c.half_cols + size, c.half_cols - size), fcols] = zeros
            else:
                w_stage[gi, size:, :] = zeros

    weight_loads(load_begin)

    smalls[2].wait()
    gain = gain_in[...].astype(jnp.float32).reshape(1, c.dz)
    for r in range(c.gain_rows):
        packs[z, r : r + 1, :] = gain[:, r * LANES : (r + 1) * LANES]
    part = roll_buf.shape[1]
    smalls[1].wait()
    tail = [roll_buf[...]] if part == LANES else [roll_buf[...], jnp.zeros((1, LANES - part), jnp.float32)]
    packs[z, c.gain_rows :, :] = jnp.broadcast_to(
        jnp.concatenate(tail, axis=1), (8 - c.gain_rows, LANES)
    )
    m_buf[...] = jnp.full(m_buf.shape, LOW, jnp.float32)
    for ref in (l_buf, q_buf, p_buf):
        ref[...] = jnp.zeros(ref.shape, jnp.float32)
    smalls[0].wait()
    ids_all[g] = id_buf[...]
    load_x.wait()

    neighbours = jnp.where(has_right, 1, 0) + jnp.where(has_left, 1, 0)
    pl.semaphore_wait(barrier, len(peers) + neighbours)

    def piece(gi, q, zi):
        return x_buf.at[
            gi, pl.ds(pl.multiple_of(q * c.rows, c.rows), c.rows), pl.ds(pl.multiple_of(zi * c.dz, c.dz), c.dz)
        ]

    def w_block(fi, h, j):
        return w_full.at[
            pl.ds(pl.multiple_of(h * c.half_cols + j * c.chunk, c.chunk), c.chunk),
            pl.ds(pl.multiple_of(fi * c.kr, c.kr), c.kr),
        ]

    def y_tokens(n, act):
        for d in range(1, G):
            q = n - (G - d) * T

            @pl.when((q >= 0) & (q < T))
            def _(d=d, q=q):
                act(remote(piece(g, q, z), piece(g, q, z), y_send.at[d - 1], y_recv.at[G - d - 1, q], dev_g(group(d))))

    def y_weights(j, act):
        for d in range(1, G):
            gi = group(d)
            src = w_stage.at[gi, pl.ds(pl.multiple_of(j * c.chunk, c.chunk), c.chunk), :]
            act(remote(src, w_block(f, x, j), wy_send.at[d - 1], wy_recv.at[G - d - 1, j], dev_g(gi)))

    def hop_ends(s):
        return ((z - s >= 0, jnp.maximum(z - s, 0), has_right, right_dev, right_send, pack_right),
                (z + s < Z, jnp.minimum(z + s, Z - 1), has_left, left_dev, left_send, pack_left))

    def locate(n):
        return group(n // T), lax.rem(n, T), lax.rem(n, Z_RING)

    def hop_wait(n, s):
        gi, q, slot = locate(n)
        if s == 0:
            @pl.when(n >= T)
            def _():
                arrive(piece(gi, q, z), y_recv.at[n // T - 1, q])
            return
        for ok, zi, _, _, _, _ in hop_ends(s):
            @pl.when(ok)
            def _():
                arrive(piece(gi, q, zi), tok_recv.at[slot, zi])

    def hop_send(n, s, act):
        gi, q, slot = locate(n)
        for ok, zi, has, dev, sem, _ in hop_ends(s):
            @pl.when(ok & has)
            def _():
                act(remote(piece(gi, q, zi), piece(gi, q, zi), sem.at[zi], tok_recv.at[slot, zi], dev))

    def pack_wait(s):
        for ok, zi, _, _, _, _ in hop_ends(s):
            @pl.when(ok)
            def _():
                arrive(packs.at[zi], pack_recv.at[zi])

    def pack_hop(s, act):
        for ok, zi, has, dev, _, sem in hop_ends(s):
            @pl.when(ok & has)
            def _():
                act(remote(packs.at[zi], packs.at[zi], sem.at[zi], pack_recv.at[zi], dev))

    def core_pass(src, fi, h, j, act):
        gi = fi // 2
        act(remote(src, w_block(fi, h, j), core_send.at[gi, h], core_recv.at[j], partner))

    def x_weights(d, fi, j, act):
        for dx in range(1, DP):
            act(remote(w_block(fi, x, j), w_block(fi, x, j), wx_send.at[d - 1, dx - 1],
                       wx_recv.at[d - 1, DP - dx - 1, j], dev_x(lax.rem(x + dx, DP))))

    def ids_move(act):
        for d in range(1, G):
            act(remote(id_buf, ids_all.at[g], ids_send.at[d - 1], ids_recv.at[G - d - 1], dev_g(group(d))))

    def roll_move(act):
        for dx in range(DP):
            for df in range(F):
                if dx or df:
                    act(remote(row_buf, roll.at[me_resp], roll_send, roll_recv,
                               (lax.rem(x + dx, DP), lax.rem(f + df, F), z)))

    def stats_move(p, late, act):
        d, half = p // c.group_pairs, lax.rem(p, c.group_pairs)
        gi = group(d)
        for s in range(Z - 1, -1, -1):
            def go(s=s):
                act(remote(s_out.at[p], s_all.at[half * (G * Z) + g * Z + z], st_send.at[late], st_recv.at[late],
                           (x, gi * 2 + core, lax.rem(z + s, Z))))
            if s:
                go()
            else:
                pl.when(d > 0)(go)

    def normalize(n):
        gi, q, _ = locate(n)
        values = x_buf[gi, pl.ds(pl.multiple_of(q * c.rows, c.rows), c.rows), :].astype(jnp.float32)
        inv = lax.rsqrt(jnp.sum(values * values, axis=1, keepdims=True) / c.dim + norm_eps)
        there = pl.ds(pl.multiple_of(n * c.rows, c.rows), c.rows)
        for zi in range(Z):
            for r in range(c.gain_rows):
                here = slice(zi * c.dz + r * LANES, zi * c.dz + (r + 1) * LANES)
                scaled = values[:, here] * inv * packs[zi, r : r + 1, :]
                n_buf[there, here] = scaled.astype(jnp.bfloat16)

    def unit(p, k):
        tokens = n_buf[pl.ds(pl.multiple_of(p * c.width, c.width), c.width), :]
        index = lax.broadcasted_iota(jnp.int32, (c.unit_cols // 8, 8, 1), 0) * 8 + lax.broadcasted_iota(
            jnp.int32, (c.unit_cols // 8, 8, 1), 1
        )
        for h in range(DP):
            off = h * c.half_cols + k * c.unit_cols
            cols = pl.ds(pl.multiple_of(off, c.chunk), c.unit_cols)
            logits = lax.dot_general(
                w_full[cols, :], tokens, (((1,), (1,)), ((), ())), preferred_element_type=jnp.float32
            ).reshape(c.unit_cols // 8, 8, c.width)
            valid = c.vt - g * c.block_cols - off
            place = rel[p] - off
            p_buf[p] = p_buf[p] + jnp.sum(jnp.where(index == place[None], logits, 0.0), axis=0)
            logits = jnp.where(index < valid, logits, LOW)
            before = m_buf[p]
            top = jnp.maximum(before, jnp.max(logits, axis=0))
            scale = jnp.exp(before - top)
            e = jnp.exp(logits - top[None])
            m_buf[p] = top
            l_buf[p] = l_buf[p] * scale + jnp.sum(e, axis=0)
            q_buf[p] = q_buf[p] * (scale * scale) + jnp.sum(e * e, axis=0)

    def collect(p):
        m_p = m_buf[p]
        top = jnp.max(m_p, axis=0, keepdims=True)
        scale = jnp.exp(m_p - top)
        total = jnp.sum(l_buf[p] * scale, axis=0, keepdims=True)
        square = jnp.sum(q_buf[p] * (scale * scale), axis=0, keepdims=True)
        picked = jnp.sum(p_buf[p], axis=0, keepdims=True)
        s_out[p] = jnp.concatenate([top, total, square, picked], axis=0)

    def collect_send(p, late):
        p = jnp.int32(p)
        collect(p)
        stats_move(p, late, begin)

        @pl.when(p < c.group_pairs)
        def _():
            s_all[p * (G * Z) + g * Z + z] = s_out[p]

    pack_hop(0, begin)
    ids_move(begin)

    def wait_loads(stage):
        def act(own, size, copy, gi, h):
            if size and own != stage:
                copy().wait()
        weight_loads(act)

    def tick(i, seen):
        w_first, y_first, x_first, r_first, u_first = seen

        @pl.when(i == 0)
        def _():
            wait_loads(True)

        w_end = due(i, c.w_tick)

        @pl.when(i + LEAD < N)
        def _():
            y_tokens(i + LEAD, begin)

        @pl.loop(w_first, w_end)
        def _(j):
            y_weights(j, begin)

        for s in range(Z):
            q = i - s

            @pl.when((q >= 0) & (q < N))
            def _(s=s, q=q):
                if s:
                    @pl.when(q == 0)
                    def _():
                        pack_wait(s)
                        if s < Z - 1:
                            pack_hop(s, begin)
                hop_wait(q, s)
                if s < Z - 1:
                    hop_send(q, s, begin)

        @pl.when(i == 1)
        def _():
            wait_loads(False)

        for n in range(2):
            j = 2 * (i - 1) + n

            @pl.when((j >= 0) & (j < J))
            def _(j=j):
                for h in range(DP):
                    core_pass(w_block(f, h, j), f, h, j, begin)

        r_end = due(i, c.r_tick)

        @pl.loop(r_first, r_end)
        def _(j):
            arrive(w_full.at[pl.ds(0, G * DP * c.kr * c.chunk // c.dim), :], core_recv.at[j])

        y_end = due(i, c.y_tick)

        @pl.loop(y_first, y_end)
        def _(j):
            for d in range(1, G):
                gi = group(d)
                fi = gi * 2 + core
                arrive(w_block(fi, x, j), wy_recv.at[d - 1, j])
                x_weights(d, fi, j, begin)
                core_pass(w_block(fi, x, j), fi, x, j, begin)

        x_end = due(i, c.x_tick)

        @pl.loop(x_first, x_end)
        def _(j):
            for d in range(1, G):
                gi = group(d)
                fi = gi * 2 + core
                for dx in range(1, DP):
                    xi = lax.rem(x + dx, DP)
                    arrive(w_block(fi, xi, j), wx_recv.at[d - 1, dx - 1, j])
                    core_pass(w_block(fi, xi, j), fi, xi, j, begin)

        q = i - (Z - 1)

        @pl.when((q >= 0) & (q < N))
        def _():
            normalize(q)

        @pl.when(i == Z)
        def _():
            for zi in range(Z):
                row_buf[:, zi * part : (zi + 1) * part] = packs[zi, c.gain_rows : c.gain_rows + 1, :part]
            for d in range(1, G):
                arrive(ids_all.at[group(d)], ids_recv.at[d - 1])
            base = z * c.vt + g * c.block_cols
            for d in range(G):
                for half in range(c.group_pairs):
                    ids = ids_all[group(d), :, half * c.width : (half + 1) * c.width]
                    rel[d * c.group_pairs + half] = jnp.broadcast_to(ids - base, (8, c.width))

        u_end = lookup(i, c.counts)

        @pl.loop(u_first, u_end)
        def _(u):
            unit(lookup(u, [p for p, _ in c.order]), lookup(u, [k for _, k in c.order]))

        return w_end, y_end, x_end, r_end, u_end

    lax.fori_loop(0, c.ticks, tick, (jnp.int32(0),) * 5)
    roll_move(begin)
    pl.loop(0, c.pairs - 1)(lambda p: collect_send(p, 0))
    pl.loop(0, c.blocks)(lambda k: unit(c.pairs - 1, k))
    collect_send(c.pairs - 1, 1)

    for copy in smalls[3:]:
        copy.wait()
    def done(ref, sem):
        remote(ref, ref, sem, sem, partner).wait_send()

    def features(gi, zi):
        return x_buf.at[gi, :, pl.ds(pl.multiple_of(zi * c.dz, c.dz), c.dz)]

    stage = w_stage.at[0]
    for d in range(1, G):
        done(features(g, z), y_send.at[d - 1])
        done(stage, wy_send.at[d - 1])
        for dx in range(1, DP):
            done(stage, wx_send.at[d - 1, dx - 1])
    for gi in range(G):
        for h in range(DP):
            done(stage, core_send.at[gi, h])
    for zi in range(Z):
        for cond, sem in (((zi <= z) & has_right, right_send), ((zi >= z) & has_left, left_send)):
            @pl.when(cond)
            def _():
                done(x_buf.at[:, :, pl.ds(zi * c.dz, c.dz)], sem.at[zi])

    for s in range(Z - 1):
        pack_hop(s, sent)
    ids_move(sent)
    roll[me_resp] = row_buf[...]
    arrive(roll.at[pl.ds(0, c.resp - 1)], roll_recv)
    ref = jnp.zeros((1, c.tok), jnp.float32)
    row = row_in[...]
    for r in range(c.resp):
        ref = ref + jnp.where(row == r, roll[r], 0.0)
    position = lax.broadcasted_iota(jnp.int32, (1, c.tok), 1)
    live = jnp.where(position < len_in[...], 1.0, 0.0)
    old, adv = old_buf[...], adv_buf[...]

    early = c.group_pairs * (G * Z - 1) - Z
    arrive(s_all.at[pl.ds(0, early)], st_recv.at[0])
    arrive(s_all.at[pl.ds(0, Z)], st_recv.at[1])
    every = [(gi, zi) for gi in range(G) for zi in range(Z)]

    def stat(gi, zi, k):
        return jnp.concatenate([s_all[p * (G * Z) + gi * Z + zi, k : k + 1, :] for p in range(c.group_pairs)], axis=1)

    top = stat(0, 0, 0)
    for gi, zi in every[1:]:
        top = jnp.maximum(top, stat(gi, zi, 0))
    total = square = picked = jnp.zeros((1, c.tok), jnp.float32)
    for gi, zi in every:
        scale = jnp.exp(stat(gi, zi, 0) - top)
        total = total + stat(gi, zi, 1) * scale
        square = square + stat(gi, zi, 2) * (scale * scale)
        picked = picked + stat(gi, zi, 3)
    new_logp = picked - top - jnp.log(total)
    prob_square = square / (total * total)
    token_loss, kl_part, grad_part = token_terms(new_logp, old, adv, ref, live, prob_square)
    sums = [jnp.sum(v, axis=1, keepdims=True) for v in (live, token_loss, kl_part, grad_part)]
    t_out[...] = jnp.concatenate(
        [jnp.broadcast_to(v, (1, LANES)) for v in sums] + [jnp.zeros((4, LANES), jnp.float32)], axis=0
    )

    def totals_move(act):
        for dx in range(DP):
            for df in range(F):
                if dx or df:
                    act(remote(t_out, t_in.at[me_resp], tot_send, tot_recv,
                               (lax.rem(x + dx, DP), lax.rem(f + df, F), z)))

    totals_move(begin)
    t_in[me_resp] = t_out[...]
    out[0:1, :] = new_logp
    out[1:2, :] = token_loss
    out[3:8, :] = jnp.zeros((5, c.tok), jnp.float32)
    done(roll.at[pl.ds(0, c.resp - 1)], roll_send)
    done(s_all.at[pl.ds(0, early)], st_send.at[0])
    done(s_all.at[pl.ds(0, Z)], st_send.at[1])
    arrive(t_in.at[pl.ds(0, c.resp - 1)], tot_recv)
    totals = sum(t_in[r] for r in range(c.resp))
    count = totals[0:1]
    lane = lax.broadcasted_iota(jnp.int32, (1, LANES), 1)
    means = jnp.where(lane == 0, totals[1:2] / count,
                      jnp.where(lane == 1, totals[2:3] / count, jnp.sqrt(totals[3:4] / count)))
    out[2:3, :] = jnp.concatenate([means] * (c.tok // LANES), axis=1)
    done(t_in.at[pl.ds(0, c.resp - 1)], tot_send)


def split(src, logp, loss, summary):
    logp[...] = src[0:1, :]
    loss[...] = src[1:2, :]
    summary[...] = src[2:3, 0:3].reshape(3)


def shards(c_of, hidden, norm_gain, head_weight, token_ids, lengths, old_logp, advantages, rollout_logp, rollout_row):
    c = c_of(hidden.shape[0], hidden.shape[1], head_weight.shape[0], head_weight.shape[1])
    G, Z, DP, F, T, J = c.groups, c.tz, c.dp, c.fs, c.group_steps, c.chunks
    vmem = pl.BlockSpec(memory_space=pltpu.VMEM)
    hbm = pl.BlockSpec(memory_space=pl.ANY)
    dma = lambda *shape: pltpu.SemaphoreType.DMA(shape)
    one_sem = pltpu.SemaphoreType.DMA
    f32, i32, b16 = jnp.float32, jnp.int32, jnp.bfloat16
    one = lambda dtype, lead=(): pltpu.VMEM((*lead, 1, c.tok), dtype)
    lanes = lambda dtype: pltpu.VMEM((c.pairs, 8, c.width), dtype)
    out = pl.pallas_call(
        functools.partial(kernel, c),
        out_shape=jax.ShapeDtypeStruct((8, c.tok), f32),
        in_specs=[hbm] * 9,
        out_specs=vmem,
        scratch_shapes=[
            one(i32), pltpu.VMEM(rollout_logp.shape, f32), one(f32), one(f32),
            pltpu.VMEM(norm_gain.shape, b16), pltpu.VMEM((1, 1), i32), pltpu.VMEM((1, 1), i32),
            pltpu.VMEM((G, c.tok, c.dim), b16),
            pltpu.VMEM((c.pairs * c.width, c.dim), b16),
            pltpu.VMEM((G, c.half_cols, c.kr), b16),
            pltpu.VMEM((c.block_cols, c.dim), b16),
            pltpu.VMEM((Z, 8, LANES), f32),
            one(i32, (G,)),
            lanes(i32), lanes(f32), lanes(f32), lanes(f32), lanes(f32),
            one(f32), one(f32, (c.resp,)),
            pltpu.VMEM((c.pairs, 4, c.width), f32),
            pltpu.VMEM((c.group_pairs * G * Z, 4, c.width), f32),
            pltpu.VMEM((8, LANES), f32),
            pltpu.VMEM((c.resp, 8, LANES), f32),
            dma(7), one_sem, dma(G), dma(DP), dma(Z_RING, Z), dma(G - 1, T), dma(G - 1), dma(Z), dma(Z),
            dma(G - 1), dma(G - 1, J), dma(G - 1, DP - 1), dma(G - 1, DP - 1, J), dma(G, DP), dma(J),
            dma(G - 1), dma(G - 1), dma(Z), dma(Z), dma(Z), one_sem, one_sem,
            dma(2), dma(2), one_sem, one_sem,
        ],
        compiler_params=pltpu.CompilerParams(
            collective_id=0, has_side_effects=True, vmem_limit_bytes=64 * 1024 * 1024 - 65536
        ),
    )(hidden, norm_gain, head_weight.T, token_ids, rollout_logp, old_logp, advantages,
      lengths.reshape(1, 1), rollout_row.reshape(1, 1))
    row = lambda n: jax.ShapeDtypeStruct((1, c.tok), f32)
    return pl.pallas_call(
        split,
        out_shape=(row(0), row(1), jax.ShapeDtypeStruct((3,), f32)),
        in_specs=[vmem],
        out_specs=(vmem, vmem, vmem),
    )(out)


def solution(mesh):
    rows = ("dp", "fsdp")
    in_specs = (
        P(rows, "tensor"), P("tensor"), P("fsdp", "tensor"), P(rows, None), P(rows),
        P(rows, None), P(rows, None), P(rows, "tensor"), P(rows),
    )
    out_specs = (P(rows, None), P(rows, None), P())
    return jax.shard_map(
        functools.partial(shards, functools.partial(Config, mesh)),
        mesh=mesh, in_specs=in_specs, out_specs=out_specs, check_vma=False,
    )
```

```python
import functools

import jax
import jax.numpy as jnp
from jax import lax
from jax.experimental import pallas as pl
from jax.experimental.pallas import tpu as pltpu
from jax.sharding import PartitionSpec as P

MESH = pl.DeviceIdType.MESH
clip_eps = 0.2
kl_coef = 0.2
log_limit = 10.0
norm_eps = 1e-06
LANES = 128
LOW = -1e30
UNITS_PER_TICK = 2
LEAD = 5
Z_RING = 4
TICK, FILL, W_STEP, W_AHEAD, Y_HEAD, Y_LAG, X_LAG, SLACK = 4.25, 3.8, 2.8, 12.0, 7.5, 3.5, 2.4, 1.5


def token_terms(new_logp, old_logp, advantages, ref_logp, live_mask, prob_square):
    shift = new_logp - old_logp
    prob_ratio = jnp.exp(jnp.clip(shift, -log_limit, log_limit))
    clipped = jnp.clip(prob_ratio, 1.0 - clip_eps, 1.0 + clip_eps)
    plain_term = prob_ratio * advantages
    bounded_term = clipped * advantages
    surrogate = jnp.minimum(plain_term, bounded_term)
    ref_gap = ref_logp - new_logp
    gap_clip = jnp.clip(ref_gap, -log_limit, log_limit)
    gap_exp = jnp.exp(gap_clip)
    kl_term = gap_exp - gap_clip - 1.0
    token_loss = live_mask * (kl_coef * kl_term - surrogate)
    gap_part = jnp.where(jnp.abs(ref_gap) < log_limit, kl_coef * (1.0 - gap_exp), 0.0)
    active = (plain_term <= bounded_term) & (jnp.abs(shift) < log_limit)
    grad_coef = live_mask * (gap_part - jnp.where(active, plain_term, 0.0))
    grad_square = grad_coef * grad_coef * (prob_square - 2.0 * jnp.exp(new_logp) + 1.0)
    return (token_loss, live_mask * kl_term, grad_square)


class Config:
    def __init__(self, mesh, tok, dz, kr, vt):
        self.dp, self.fs, self.tz = (mesh.shape[a] for a in ("dp", "fsdp", "tensor"))
        self.groups = self.fs // 2
        self.tok, self.dz, self.kr, self.vt = tok, dz, kr, vt
        self.dim = dz * self.tz
        self.resp = self.dp * self.fs
        tiles = -(-vt // LANES)
        self.half_tiles = -(-tiles // (self.groups * self.dp))
        self.half_cols = self.half_tiles * LANES
        self.block_cols = self.half_cols * self.dp
        self.rows = 64
        self.group_steps = tok // self.rows
        self.steps = self.groups * self.group_steps
        self.chunks = max(j for j in range(1, 17) if self.half_tiles % j == 0)
        self.chunk = self.half_cols // self.chunks
        self.width = 256
        self.per_pair = self.width // self.rows
        self.group_pairs = tok // self.width
        self.pairs = self.groups * self.group_pairs
        self.span = next(n for n in (4, 2, 1) if self.chunks % n == 0)
        self.blocks = self.chunks // self.span
        self.unit_cols = self.span * self.chunk
        self.gain_rows = dz // LANES
        self.plan()

    def plan(self):
        N, Z, J, T = self.steps, self.tz, self.chunks, self.group_steps
        self.ticks = N + Z - 1
        last = self.ticks - 1
        at = [FILL * n for n in range(Z)]
        for n in range(Z, self.ticks):
            at.append(at[-1] + TICK * sum(0 <= n - 1 - h < N for h in range(Z - 1)) / (Z - 1))

        def tick_at(t, low):
            return min([n for n in range(low, last) if at[n] >= t - SLACK], default=last)

        step = W_STEP * N / J
        alone = max(1, int((T * TICK - Y_HEAD) / step))
        self.w_tick, self.y_tick, self.x_tick, self.r_tick = [], [], [], []
        x_free = 0.0
        for j in range(J):
            begin = step * j if j < alone else step * alone + (j - alone) * TICK + TICK / 3
            self.w_tick.append(max(n for n in range(last) if n == 0 or at[n] <= begin - W_AHEAD))
            y = tick_at(begin + step + Y_LAG, self.w_tick[-1] + 1)
            x_free = max(x_free, at[y]) + step
            x = tick_at(x_free + X_LAG, y + 1)
            r = min(last, x + 1)
            self.y_tick.append(y)
            self.x_tick.append(x)
            self.r_tick.append(r)
        done, self.order, self.counts = set(), [], []
        for i in range(self.ticks):
            n = 0
            for k in range(self.blocks):
                for p in range(self.pairs - 1):
                    if (p, k) in done or (p + 1) * self.per_pair + Z - 2 > i or self.r_tick[(k + 1) * self.span - 1] > i:
                        continue
                    if n < UNITS_PER_TICK or i >= last:
                        done.add((p, k))
                        self.order.append((p, k))
                        n += 1
            self.counts.append(len(self.order))


def lookup(index, table):
    value = jnp.int32(table[0])
    for t in range(1, len(table)):
        if table[t] != table[t - 1]:
            value = value + jnp.where(index >= t, table[t] - table[t - 1], 0)
    return value


def due(i, ticks):
    count = jnp.int32(0)
    for t in ticks:
        count = count + jnp.where(i >= t, 1, 0)
    return count


def kernel(
    c,
    hid, gain_any, w_any, id_any, roll_any, old_any, adv_any, len_any, row_any,
    out,
    id_buf, roll_buf, old_buf, adv_buf, gain_in, len_in, row_in,
    x_buf, n_buf, w_stage, w_full, packs, ids_all, rel, m_buf, l_buf, q_buf, p_buf,
    row_buf, roll, s_out, s_all, t_out, t_in,
    small_sem, x_sem, stage_sem, own_sem, tok_recv, y_recv, y_send, right_send, left_send,
    wy_send, wy_recv, wx_send, wx_recv, core_send, core_recv,
    ids_send, ids_recv, pack_right, pack_left, pack_recv, roll_send, roll_recv,
    st_send, st_recv, tot_send, tot_recv,
):
    G, Z, DP, F, N, T, J = c.groups, c.tz, c.dp, c.fs, c.steps, c.group_steps, c.chunks
    x = lax.axis_index("dp")
    f = lax.axis_index("fsdp")
    z = lax.axis_index("tensor")
    g, core = f // 2, f % 2
    partner = (x, g * 2 + (1 - core), z)
    me_resp = x * F + f
    right_dev = (x, f, jnp.minimum(z + 1, Z - 1))
    left_dev = (x, f, jnp.maximum(z - 1, 0))
    has_right, has_left = z + 1 < Z, z >= 1

    def dev_g(gi):
        return (x, gi * 2 + core, z)

    def dev_x(xi):
        return (xi, f, z)

    def group(d):
        return lax.rem(g + d, G)

    def remote(src, dst, ss, rs, dev):
        return pltpu.make_async_remote_copy(
            src_ref=src, dst_ref=dst, send_sem=ss, recv_sem=rs, device_id=dev, device_id_type=MESH
        )

    def arrive(dst, rs):
        remote(dst, dst, rs, rs, partner).wait_recv()

    def begin(copy):
        copy.start()

    def sent(copy):
        copy.wait_send()

    barrier = pltpu.get_barrier_semaphore()
    peers = [dev_g(group(d)) for d in range(1, G)] + [partner]
    peers += [dev_x(lax.rem(x + d, DP)) for d in range(1, DP)]
    for dev in peers:
        pl.semaphore_signal(barrier, inc=1, device_id=dev, device_id_type=MESH)
    for cond, dev in ((has_right, right_dev), (has_left, left_dev)):
        @pl.when(cond)
        def _(dev=dev):
            pl.semaphore_signal(barrier, inc=1, device_id=dev, device_id_type=MESH)

    zcols = pl.ds(pl.multiple_of(z * c.dz, c.dz), c.dz)
    fcols = pl.ds(pl.multiple_of(f * c.kr, c.kr), c.kr)
    load_x = pltpu.make_async_copy(hid, x_buf.at[g, :, zcols], x_sem)
    load_x.start()
    smalls = [
        pltpu.make_async_copy(a, b, small_sem.at[n])
        for n, (a, b) in enumerate(
            ((id_any, id_buf), (roll_any, roll_buf), (gain_any, gain_in), (old_any, old_buf), (adv_any, adv_buf),
             (len_any, len_in), (row_any, row_in))
        )
    ]
    for copy in smalls:
        copy.start()

    def weight_loads(act):
        for own in (False, True):
            for gi in range(G):
                for h in range(DP):
                    start = gi * c.block_cols + h * c.half_cols
                    size = max(0, min(c.half_cols, c.vt - start))
                    src = w_any.at[pl.ds(start, size), :]

                    @pl.when(gi == g if own else (gi != g) & (x == h))
                    def _():
                        if own:
                            dst, sem = w_full.at[pl.ds(h * c.half_cols, size), fcols], own_sem.at[h]
                        else:
                            dst, sem = w_stage.at[gi, pl.ds(0, size), :], stage_sem.at[gi]
                        act(own, size, lambda: pltpu.make_async_copy(src, dst, sem), gi, h)

    def load_begin(own, size, copy, gi, h):
        if size:
            copy().start()
        if size < c.half_cols:
            zeros = jnp.zeros((c.half_cols - size, c.kr), w_full.dtype)
            if own:
                w_full[pl.ds(h * c.half_cols + size, c.half_cols - size), fcols] = zeros
            else:
                w_stage[gi, size:, :] = zeros

    weight_loads(load_begin)

    smalls[2].wait()
    gain = gain_in[...].astype(jnp.float32).reshape(1, c.dz)
    for r in range(c.gain_rows):
        packs[z, r : r + 1, :] = gain[:, r * LANES : (r + 1) * LANES]
    part = roll_buf.shape[1]
    smalls[1].wait()
    tail = [roll_buf[...]] if part == LANES else [roll_buf[...], jnp.zeros((1, LANES - part), jnp.float32)]
    packs[z, c.gain_rows :, :] = jnp.broadcast_to(
        jnp.concatenate(tail, axis=1), (8 - c.gain_rows, LANES)
    )
    m_buf[...] = jnp.full(m_buf.shape, LOW, jnp.float32)
    for ref in (l_buf, q_buf, p_buf):
        ref[...] = jnp.zeros(ref.shape, jnp.float32)
    smalls[0].wait()
    ids_all[g] = id_buf[...]
    load_x.wait()

    neighbours = jnp.where(has_right, 1, 0) + jnp.where(has_left, 1, 0)
    pl.semaphore_wait(barrier, len(peers) + neighbours)

    def piece(gi, q, zi):
        return x_buf.at[
            gi, pl.ds(pl.multiple_of(q * c.rows, c.rows), c.rows), pl.ds(pl.multiple_of(zi * c.dz, c.dz), c.dz)
        ]

    def w_block(fi, h, j):
        return w_full.at[
            pl.ds(pl.multiple_of(h * c.half_cols + j * c.chunk, c.chunk), c.chunk),
            pl.ds(pl.multiple_of(fi * c.kr, c.kr), c.kr),
        ]

    def y_tokens(n, act):
        for d in range(1, G):
            q = n - (G - d) * T

            @pl.when((q >= 0) & (q < T))
            def _(d=d, q=q):
                act(remote(piece(g, q, z), piece(g, q, z), y_send.at[d - 1], y_recv.at[G - d - 1, q], dev_g(group(d))))

    def y_weights(j, act):
        for d in range(1, G):
            gi = group(d)
            src = w_stage.at[gi, pl.ds(pl.multiple_of(j * c.chunk, c.chunk), c.chunk), :]
            act(remote(src, w_block(f, x, j), wy_send.at[d - 1], wy_recv.at[G - d - 1, j], dev_g(gi)))

    def hop_ends(s):
        return ((z - s >= 0, jnp.maximum(z - s, 0), has_right, right_dev, right_send, pack_right),
                (z + s < Z, jnp.minimum(z + s, Z - 1), has_left, left_dev, left_send, pack_left))

    def locate(n):
        return group(n // T), lax.rem(n, T), lax.rem(n, Z_RING)

    def hop_wait(n, s):
        gi, q, slot = locate(n)
        if s == 0:
            @pl.when(n >= T)
            def _():
                arrive(piece(gi, q, z), y_recv.at[n // T - 1, q])
            return
        for ok, zi, _, _, _, _ in hop_ends(s):
            @pl.when(ok)
            def _():
                arrive(piece(gi, q, zi), tok_recv.at[slot, zi])

    def hop_send(n, s, act):
        gi, q, slot = locate(n)
        for ok, zi, has, dev, sem, _ in hop_ends(s):
            @pl.when(ok & has)
            def _():
                act(remote(piece(gi, q, zi), piece(gi, q, zi), sem.at[zi], tok_recv.at[slot, zi], dev))

    def pack_wait(s):
        for ok, zi, _, _, _, _ in hop_ends(s):
            @pl.when(ok)
            def _():
                arrive(packs.at[zi], pack_recv.at[zi])

    def pack_hop(s, act):
        for ok, zi, has, dev, _, sem in hop_ends(s):
            @pl.when(ok & has)
            def _():
                act(remote(packs.at[zi], packs.at[zi], sem.at[zi], pack_recv.at[zi], dev))

    def core_pass(src, fi, h, j, act):
        gi = fi // 2
        act(remote(src, w_block(fi, h, j), core_send.at[gi, h], core_recv.at[j], partner))

    def x_weights(d, fi, j, act):
        for dx in range(1, DP):
            act(remote(w_block(fi, x, j), w_block(fi, x, j), wx_send.at[d - 1, dx - 1],
                       wx_recv.at[d - 1, DP - dx - 1, j], dev_x(lax.rem(x + dx, DP))))

    def ids_move(act):
        for d in range(1, G):
            act(remote(id_buf, ids_all.at[g], ids_send.at[d - 1], ids_recv.at[G - d - 1], dev_g(group(d))))

    def roll_move(act):
        for dx in range(DP):
            for df in range(F):
                if dx or df:
                    act(remote(row_buf, roll.at[me_resp], roll_send, roll_recv,
                               (lax.rem(x + dx, DP), lax.rem(f + df, F), z)))

    def stats_move(p, late, act):
        d, half = p // c.group_pairs, lax.rem(p, c.group_pairs)
        gi = group(d)
        for s in range(Z - 1, -1, -1):
            def go(s=s):
                act(remote(s_out.at[p], s_all.at[half * (G * Z) + g * Z + z], st_send.at[late], st_recv.at[late],
                           (x, gi * 2 + core, lax.rem(z + s, Z))))
            if s:
                go()
            else:
                pl.when(d > 0)(go)

    def normalize(n):
        gi, q, _ = locate(n)
        values = x_buf[gi, pl.ds(pl.multiple_of(q * c.rows, c.rows), c.rows), :].astype(jnp.float32)
        inv = lax.rsqrt(jnp.sum(values * values, axis=1, keepdims=True) / c.dim + norm_eps)
        there = pl.ds(pl.multiple_of(n * c.rows, c.rows), c.rows)
        for zi in range(Z):
            for r in range(c.gain_rows):
                here = slice(zi * c.dz + r * LANES, zi * c.dz + (r + 1) * LANES)
                scaled = values[:, here] * inv * packs[zi, r : r + 1, :]
                n_buf[there, here] = scaled.astype(jnp.bfloat16)

    def unit(p, k, halves=None, span_cols=None):
        n_cols = span_cols or c.unit_cols
        tokens = n_buf[pl.ds(pl.multiple_of(p * c.width, c.width), c.width), :]
        index = lax.broadcasted_iota(jnp.int32, (n_cols // 8, 8, 1), 0) * 8 + lax.broadcasted_iota(
            jnp.int32, (n_cols // 8, 8, 1), 1
        )
        for h in (range(DP) if halves is None else halves):
            off = h * c.half_cols + k * n_cols
            cols = pl.ds(pl.multiple_of(off, c.chunk), n_cols)
            logits = lax.dot_general(
                w_full[cols, :], tokens, (((1,), (1,)), ((), ())), preferred_element_type=jnp.float32
            ).reshape(n_cols // 8, 8, c.width)
            valid = c.vt - g * c.block_cols - off
            place = rel[p] - off
            p_buf[p] = p_buf[p] + jnp.sum(jnp.where(index == place[None], logits, 0.0), axis=0)
            if (G - 1) * c.block_cols + (h + 1) * c.half_cols > c.vt:
                logits = jnp.where(index < valid, logits, LOW)
            before = m_buf[p]
            top = jnp.maximum(before, jnp.max(logits, axis=0))
            scale = jnp.exp(before - top)
            e = jnp.exp(logits - top[None])
            m_buf[p] = top
            l_buf[p] = l_buf[p] * scale + jnp.sum(e, axis=0)
            q_buf[p] = q_buf[p] * (scale * scale) + jnp.sum(e * e, axis=0)

    def collect(p):
        m_p = m_buf[p]
        top = jnp.max(m_p, axis=0, keepdims=True)
        scale = jnp.exp(m_p - top)
        total = jnp.sum(l_buf[p] * scale, axis=0, keepdims=True)
        square = jnp.sum(q_buf[p] * (scale * scale), axis=0, keepdims=True)
        picked = jnp.sum(p_buf[p], axis=0, keepdims=True)
        s_out[p] = jnp.concatenate([top, total, square, picked], axis=0)

    def collect_send(p, late):
        p = jnp.int32(p)
        collect(p)
        stats_move(p, late, begin)

        @pl.when(p < c.group_pairs)
        def _():
            s_all[p * (G * Z) + g * Z + z] = s_out[p]

    pack_hop(0, begin)
    ids_move(begin)

    def wait_loads(stage):
        def act(own, size, copy, gi, h):
            if size and own != stage:
                copy().wait()
        weight_loads(act)

    def tick(i, seen):
        w_first, y_first, x_first, r_first, u_first = seen

        @pl.when(i == 0)
        def _():
            wait_loads(True)

        w_end = due(i, c.w_tick)

        @pl.when(i + LEAD < N)
        def _():
            y_tokens(i + LEAD, begin)

        @pl.loop(w_first, w_end)
        def _(j):
            y_weights(j, begin)

        for s in range(Z):
            q = i - s

            @pl.when((q >= 0) & (q < N))
            def _(s=s, q=q):
                if s:
                    @pl.when(q == 0)
                    def _():
                        pack_wait(s)
                        if s < Z - 1:
                            pack_hop(s, begin)
                hop_wait(q, s)
                if s < Z - 1:
                    hop_send(q, s, begin)

        @pl.when(i == 1)
        def _():
            wait_loads(False)

        for n in range(2):
            j = 2 * (i - 1) + n

            @pl.when((j >= 0) & (j < J))
            def _(j=j):
                for h in range(DP):
                    core_pass(w_block(f, h, j), f, h, j, begin)

        r_end = due(i, c.r_tick)

        @pl.loop(r_first, r_end)
        def _(j):
            arrive(w_full.at[pl.ds(0, G * DP * c.kr * c.chunk // c.dim), :], core_recv.at[j])

        y_end = due(i, c.y_tick)

        @pl.loop(y_first, y_end)
        def _(j):
            for d in range(1, G):
                gi = group(d)
                fi = gi * 2 + core
                arrive(w_block(fi, x, j), wy_recv.at[d - 1, j])
                x_weights(d, fi, j, begin)
                core_pass(w_block(fi, x, j), fi, x, j, begin)

        x_end = due(i, c.x_tick)

        @pl.loop(x_first, x_end)
        def _(j):
            for d in range(1, G):
                gi = group(d)
                fi = gi * 2 + core
                for dx in range(1, DP):
                    xi = lax.rem(x + dx, DP)
                    arrive(w_block(fi, xi, j), wx_recv.at[d - 1, dx - 1, j])
                    core_pass(w_block(fi, xi, j), fi, xi, j, begin)

        q = i - (Z - 1)

        @pl.when((q >= 0) & (q < N))
        def _():
            normalize(q)

        @pl.when(i == Z)
        def _():
            for zi in range(Z):
                row_buf[:, zi * part : (zi + 1) * part] = packs[zi, c.gain_rows : c.gain_rows + 1, :part]
            for d in range(1, G):
                arrive(ids_all.at[group(d)], ids_recv.at[d - 1])
            base = z * c.vt + g * c.block_cols
            for d in range(G):
                for half in range(c.group_pairs):
                    ids = ids_all[group(d), :, half * c.width : (half + 1) * c.width]
                    rel[d * c.group_pairs + half] = jnp.broadcast_to(ids - base, (8, c.width))

        u_end = lookup(i, c.counts)

        @pl.loop(u_first, u_end)
        def _(u):
            unit(lookup(u, [p for p, _ in c.order]), lookup(u, [k for _, k in c.order]))

        return w_end, y_end, x_end, r_end, u_end

    lax.fori_loop(0, c.ticks, tick, (jnp.int32(0),) * 5)
    roll_move(begin)
    pl.loop(0, c.pairs - 1)(lambda p: collect_send(p, 0))
    wide = 2 if c.blocks % 2 == 0 else 1

    @pl.loop(0, c.blocks // wide)
    def _(k):
        for h in range(DP):
            unit(c.pairs - 1, k, (h,), wide * c.unit_cols)
    collect_send(c.pairs - 1, 1)

    for copy in smalls[3:]:
        copy.wait()
    def done(ref, sem):
        remote(ref, ref, sem, sem, partner).wait_send()

    def features(gi, zi):
        return x_buf.at[gi, :, pl.ds(pl.multiple_of(zi * c.dz, c.dz), c.dz)]

    stage = w_stage.at[0]
    for d in range(1, G):
        done(features(g, z), y_send.at[d - 1])
        done(stage, wy_send.at[d - 1])
        for dx in range(1, DP):
            done(stage, wx_send.at[d - 1, dx - 1])
    for gi in range(G):
        for h in range(DP):
            done(stage, core_send.at[gi, h])
    for zi in range(Z):
        for cond, sem in (((zi <= z) & has_right, right_send), ((zi >= z) & has_left, left_send)):
            @pl.when(cond)
            def _():
                done(x_buf.at[:, :, pl.ds(zi * c.dz, c.dz)], sem.at[zi])

    for s in range(Z - 1):
        pack_hop(s, sent)
    ids_move(sent)
    roll[me_resp] = row_buf[...]
    arrive(roll.at[pl.ds(0, c.resp - 1)], roll_recv)
    ref = jnp.zeros((1, c.tok), jnp.float32)
    row = row_in[...]
    for r in range(c.resp):
        ref = ref + jnp.where(row == r, roll[r], 0.0)
    position = lax.broadcasted_iota(jnp.int32, (1, c.tok), 1)
    live = jnp.where(position < len_in[...], 1.0, 0.0)
    old, adv = old_buf[...], adv_buf[...]

    early = c.group_pairs * (G * Z - 1) - Z
    arrive(s_all.at[pl.ds(0, early)], st_recv.at[0])
    arrive(s_all.at[pl.ds(0, Z)], st_recv.at[1])
    every = [(gi, zi) for gi in range(G) for zi in range(Z)]

    def stat(gi, zi, k):
        return jnp.concatenate([s_all[p * (G * Z) + gi * Z + zi, k : k + 1, :] for p in range(c.group_pairs)], axis=1)

    top = stat(0, 0, 0)
    for gi, zi in every[1:]:
        top = jnp.maximum(top, stat(gi, zi, 0))
    total = square = picked = jnp.zeros((1, c.tok), jnp.float32)
    for gi, zi in every:
        scale = jnp.exp(stat(gi, zi, 0) - top)
        total = total + stat(gi, zi, 1) * scale
        square = square + stat(gi, zi, 2) * (scale * scale)
        picked = picked + stat(gi, zi, 3)
    new_logp = picked - top - jnp.log(total)
    prob_square = square / (total * total)
    token_loss, kl_part, grad_part = token_terms(new_logp, old, adv, ref, live, prob_square)
    sums = [jnp.sum(v, axis=1, keepdims=True) for v in (live, token_loss, kl_part, grad_part)]
    t_out[...] = jnp.concatenate(
        [jnp.broadcast_to(v, (1, LANES)) for v in sums] + [jnp.zeros((4, LANES), jnp.float32)], axis=0
    )

    def totals_move(act):
        for dx in range(DP):
            for df in range(F):
                if dx or df:
                    act(remote(t_out, t_in.at[me_resp], tot_send, tot_recv,
                               (lax.rem(x + dx, DP), lax.rem(f + df, F), z)))

    totals_move(begin)
    t_in[me_resp] = t_out[...]
    out[0:1, :] = new_logp
    out[1:2, :] = token_loss
    out[3:8, :] = jnp.zeros((5, c.tok), jnp.float32)
    done(roll.at[pl.ds(0, c.resp - 1)], roll_send)
    done(s_all.at[pl.ds(0, early)], st_send.at[0])
    done(s_all.at[pl.ds(0, Z)], st_send.at[1])
    arrive(t_in.at[pl.ds(0, c.resp - 1)], tot_recv)
    totals = sum(t_in[r] for r in range(c.resp))
    count = totals[0:1]
    lane = lax.broadcasted_iota(jnp.int32, (1, LANES), 1)
    means = jnp.where(lane == 0, totals[1:2] / count,
                      jnp.where(lane == 1, totals[2:3] / count, jnp.sqrt(totals[3:4] / count)))
    out[2:3, :] = jnp.concatenate([means] * (c.tok // LANES), axis=1)
    done(t_in.at[pl.ds(0, c.resp - 1)], tot_send)


def split(src, logp, loss, summary):
    logp[...] = src[0:1, :]
    loss[...] = src[1:2, :]
    summary[...] = src[2:3, 0:3].reshape(3)


def shards(c_of, hidden, norm_gain, head_weight, token_ids, lengths, old_logp, advantages, rollout_logp, rollout_row):
    c = c_of(hidden.shape[0], hidden.shape[1], head_weight.shape[0], head_weight.shape[1])
    G, Z, DP, F, T, J = c.groups, c.tz, c.dp, c.fs, c.group_steps, c.chunks
    vmem = pl.BlockSpec(memory_space=pltpu.VMEM)
    hbm = pl.BlockSpec(memory_space=pl.ANY)
    dma = lambda *shape: pltpu.SemaphoreType.DMA(shape)
    one_sem = pltpu.SemaphoreType.DMA
    f32, i32, b16 = jnp.float32, jnp.int32, jnp.bfloat16
    one = lambda dtype, lead=(): pltpu.VMEM((*lead, 1, c.tok), dtype)
    lanes = lambda dtype: pltpu.VMEM((c.pairs, 8, c.width), dtype)
    out = pl.pallas_call(
        functools.partial(kernel, c),
        out_shape=jax.ShapeDtypeStruct((8, c.tok), f32),
        in_specs=[hbm] * 9,
        out_specs=vmem,
        scratch_shapes=[
            one(i32), pltpu.VMEM(rollout_logp.shape, f32), one(f32), one(f32),
            pltpu.VMEM(norm_gain.shape, b16), pltpu.VMEM((1, 1), i32), pltpu.VMEM((1, 1), i32),
            pltpu.VMEM((G, c.tok, c.dim), b16),
            pltpu.VMEM((c.pairs * c.width, c.dim), b16),
            pltpu.VMEM((G, c.half_cols, c.kr), b16),
            pltpu.VMEM((c.block_cols, c.dim), b16),
            pltpu.VMEM((Z, 8, LANES), f32),
            one(i32, (G,)),
            lanes(i32), lanes(f32), lanes(f32), lanes(f32), lanes(f32),
            one(f32), one(f32, (c.resp,)),
            pltpu.VMEM((c.pairs, 4, c.width), f32),
            pltpu.VMEM((c.group_pairs * G * Z, 4, c.width), f32),
            pltpu.VMEM((8, LANES), f32),
            pltpu.VMEM((c.resp, 8, LANES), f32),
            dma(7), one_sem, dma(G), dma(DP), dma(Z_RING, Z), dma(G - 1, T), dma(G - 1), dma(Z), dma(Z),
            dma(G - 1), dma(G - 1, J), dma(G - 1, DP - 1), dma(G - 1, DP - 1, J), dma(G, DP), dma(J),
            dma(G - 1), dma(G - 1), dma(Z), dma(Z), dma(Z), one_sem, one_sem,
            dma(2), dma(2), one_sem, one_sem,
        ],
        compiler_params=pltpu.CompilerParams(
            collective_id=0, has_side_effects=True, vmem_limit_bytes=64 * 1024 * 1024 - 65536
        ),
    )(hidden, norm_gain, head_weight.T, token_ids, rollout_logp, old_logp, advantages,
      lengths.reshape(1, 1), rollout_row.reshape(1, 1))
    row = lambda n: jax.ShapeDtypeStruct((1, c.tok), f32)
    return pl.pallas_call(
        split,
        out_shape=(row(0), row(1), jax.ShapeDtypeStruct((3,), f32)),
        in_specs=[vmem],
        out_specs=(vmem, vmem, vmem),
    )(out)


def solution(mesh):
    rows = ("dp", "fsdp")
    in_specs = (
        P(rows, "tensor"), P("tensor"), P("fsdp", "tensor"), P(rows, None), P(rows),
        P(rows, None), P(rows, None), P(rows, "tensor"), P(rows),
    )
    out_specs = (P(rows, None), P(rows, None), P())
    return jax.shard_map(
        functools.partial(shards, functools.partial(Config, mesh)),
        mesh=mesh, in_specs=in_specs, out_specs=out_specs, check_vma=False,
    )
```

```python
import functools

import jax
import jax.numpy as jnp
from jax import lax
from jax.experimental import pallas as pl
from jax.experimental.pallas import tpu as pltpu
from jax.sharding import PartitionSpec as P

MESH = pl.DeviceIdType.MESH
clip_eps = 0.2
kl_coef = 0.2
log_limit = 10.0
norm_eps = 1e-06
LANES = 128
LOW = -1e30
UNITS_PER_TICK = 2
LEAD = 5
Z_RING = 4
TICK, FILL, W_STEP, W_AHEAD, Y_HEAD, Y_LAG, X_LAG, SLACK = 4.25, 3.8, 2.8, 12.0, 7.5, 3.5, 2.4, 1.5


def token_terms(new_logp, old_logp, advantages, ref_logp, live_mask, prob_square):
    shift = new_logp - old_logp
    prob_ratio = jnp.exp(jnp.clip(shift, -log_limit, log_limit))
    clipped = jnp.clip(prob_ratio, 1.0 - clip_eps, 1.0 + clip_eps)
    plain_term = prob_ratio * advantages
    bounded_term = clipped * advantages
    surrogate = jnp.minimum(plain_term, bounded_term)
    ref_gap = ref_logp - new_logp
    gap_clip = jnp.clip(ref_gap, -log_limit, log_limit)
    gap_exp = jnp.exp(gap_clip)
    kl_term = gap_exp - gap_clip - 1.0
    token_loss = live_mask * (kl_coef * kl_term - surrogate)
    gap_part = jnp.where(jnp.abs(ref_gap) < log_limit, kl_coef * (1.0 - gap_exp), 0.0)
    active = (plain_term <= bounded_term) & (jnp.abs(shift) < log_limit)
    grad_coef = live_mask * (gap_part - jnp.where(active, plain_term, 0.0))
    grad_square = grad_coef * grad_coef * (prob_square - 2.0 * jnp.exp(new_logp) + 1.0)
    return (token_loss, live_mask * kl_term, grad_square)


class Config:
    def __init__(self, mesh, tok, dz, kr, vt):
        self.dp, self.fs, self.tz = (mesh.shape[a] for a in ("dp", "fsdp", "tensor"))
        self.groups = self.fs // 2
        self.tok, self.dz, self.kr, self.vt = tok, dz, kr, vt
        self.dim = dz * self.tz
        self.resp = self.dp * self.fs
        tiles = -(-vt // LANES)
        self.half_tiles = -(-tiles // (self.groups * self.dp))
        self.half_cols = self.half_tiles * LANES
        self.block_cols = self.half_cols * self.dp
        self.rows = 64
        self.group_steps = tok // self.rows
        self.steps = self.groups * self.group_steps
        self.chunks = max(j for j in range(1, 17) if self.half_tiles % j == 0)
        self.chunk = self.half_cols // self.chunks
        self.width = 256
        self.per_pair = self.width // self.rows
        self.group_pairs = tok // self.width
        self.pairs = self.groups * self.group_pairs
        self.span = next(n for n in (4, 2, 1) if self.chunks % n == 0)
        self.blocks = self.chunks // self.span
        self.unit_cols = self.span * self.chunk
        self.gain_rows = dz // LANES
        self.plan()

    def plan(self):
        N, Z, J, T = self.steps, self.tz, self.chunks, self.group_steps
        self.ticks = N + Z - 1
        last = self.ticks - 1
        at = [FILL * n for n in range(Z)]
        for n in range(Z, self.ticks):
            at.append(at[-1] + TICK * sum(0 <= n - 1 - h < N for h in range(Z - 1)) / (Z - 1))

        def tick_at(t, low):
            return min([n for n in range(low, last) if at[n] >= t - SLACK], default=last)

        step = W_STEP * N / J
        alone = max(1, int((T * TICK - Y_HEAD) / step))
        self.w_tick, self.y_tick, self.x_tick, self.r_tick = [], [], [], []
        x_free = 0.0
        for j in range(J):
            begin = step * j if j < alone else step * alone + (j - alone) * TICK + TICK / 3
            self.w_tick.append(max(n for n in range(last) if n == 0 or at[n] <= begin - W_AHEAD))
            y = tick_at(begin + step + Y_LAG, self.w_tick[-1] + 1)
            x_free = max(x_free, at[y]) + step
            x = tick_at(x_free + X_LAG, y + 1)
            r = min(last, x + 1)
            self.y_tick.append(y)
            self.x_tick.append(x)
            self.r_tick.append(r)
        done, self.order, self.counts = set(), [], []
        for i in range(self.ticks):
            n = 0
            for k in range(self.blocks):
                for p in range(self.pairs - 1):
                    if (p, k) in done or (p + 1) * self.per_pair + Z - 2 > i or self.r_tick[(k + 1) * self.span - 1] > i:
                        continue
                    if n < UNITS_PER_TICK or i >= last:
                        done.add((p, k))
                        self.order.append((p, k))
                        n += 1
            self.counts.append(len(self.order))


def lookup(index, table):
    value = jnp.int32(table[0])
    for t in range(1, len(table)):
        if table[t] != table[t - 1]:
            value = value + jnp.where(index >= t, table[t] - table[t - 1], 0)
    return value


def due(i, ticks):
    count = jnp.int32(0)
    for t in ticks:
        count = count + jnp.where(i >= t, 1, 0)
    return count


def kernel(
    c,
    hid, gain_any, w_any, id_any, roll_any, old_any, adv_any, len_any, row_any,
    out,
    id_buf, roll_buf, old_buf, adv_buf, gain_in, len_in, row_in,
    x_buf, n_buf, w_stage, w_full, packs, ids_all, rel, m_buf, l_buf, q_buf, p_buf,
    row_buf, roll, s_out, s_all, t_out, t_in,
    small_sem, x_sem, stage_sem, own_sem, tok_recv, y_recv, y_send, right_send, left_send,
    wy_send, wy_recv, wx_send, wx_recv, core_send, core_recv,
    ids_send, ids_recv, pack_right, pack_left, pack_recv, roll_send, roll_recv,
    st_send, st_recv, tot_send, tot_recv,
):
    G, Z, DP, F, N, T, J = c.groups, c.tz, c.dp, c.fs, c.steps, c.group_steps, c.chunks
    x = lax.axis_index("dp")
    f = lax.axis_index("fsdp")
    z = lax.axis_index("tensor")
    g, core = f // 2, f % 2
    partner = (x, g * 2 + (1 - core), z)
    me_resp = x * F + f
    right_dev = (x, f, jnp.minimum(z + 1, Z - 1))
    left_dev = (x, f, jnp.maximum(z - 1, 0))
    has_right, has_left = z + 1 < Z, z >= 1

    def dev_g(gi):
        return (x, gi * 2 + core, z)

    def dev_x(xi):
        return (xi, f, z)

    def group(d):
        return lax.rem(g + d, G)

    def remote(src, dst, ss, rs, dev):
        return pltpu.make_async_remote_copy(
            src_ref=src, dst_ref=dst, send_sem=ss, recv_sem=rs, device_id=dev, device_id_type=MESH
        )

    def arrive(dst, rs):
        remote(dst, dst, rs, rs, partner).wait_recv()

    def begin(copy):
        copy.start()

    def sent(copy):
        copy.wait_send()

    barrier = pltpu.get_barrier_semaphore()
    peers = [dev_g(group(d)) for d in range(1, G)] + [partner]
    peers += [dev_x(lax.rem(x + d, DP)) for d in range(1, DP)]
    for dev in peers:
        pl.semaphore_signal(barrier, inc=1, device_id=dev, device_id_type=MESH)
    for cond, dev in ((has_right, right_dev), (has_left, left_dev)):
        @pl.when(cond)
        def _(dev=dev):
            pl.semaphore_signal(barrier, inc=1, device_id=dev, device_id_type=MESH)

    zcols = pl.ds(pl.multiple_of(z * c.dz, c.dz), c.dz)
    fcols = pl.ds(pl.multiple_of(f * c.kr, c.kr), c.kr)
    load_x = pltpu.make_async_copy(hid, x_buf.at[g, :, zcols], x_sem)
    load_x.start()
    smalls = [
        pltpu.make_async_copy(a, b, small_sem.at[n])
        for n, (a, b) in enumerate(
            ((id_any, id_buf), (roll_any, roll_buf), (gain_any, gain_in), (old_any, old_buf), (adv_any, adv_buf),
             (len_any, len_in), (row_any, row_in))
        )
    ]
    for copy in smalls:
        copy.start()

    def weight_loads(act):
        for own in (False, True):
            for gi in range(G):
                for h in range(DP):
                    start = gi * c.block_cols + h * c.half_cols
                    size = max(0, min(c.half_cols, c.vt - start))
                    src = w_any.at[pl.ds(start, size), :]

                    @pl.when(gi == g if own else (gi != g) & (x == h))
                    def _():
                        if own:
                            dst, sem = w_full.at[pl.ds(h * c.half_cols, size), fcols], own_sem.at[h]
                        else:
                            dst, sem = w_stage.at[gi, pl.ds(0, size), :], stage_sem.at[gi]
                        act(own, size, lambda: pltpu.make_async_copy(src, dst, sem), gi, h)

    def load_begin(own, size, copy, gi, h):
        if size:
            copy().start()
        if size < c.half_cols:
            zeros = jnp.zeros((c.half_cols - size, c.kr), w_full.dtype)
            if own:
                w_full[pl.ds(h * c.half_cols + size, c.half_cols - size), fcols] = zeros
            else:
                w_stage[gi, size:, :] = zeros

    weight_loads(load_begin)

    smalls[2].wait()
    gain = gain_in[...].astype(jnp.float32).reshape(1, c.dz)
    for r in range(c.gain_rows):
        packs[z, r : r + 1, :] = gain[:, r * LANES : (r + 1) * LANES]
    part = roll_buf.shape[1]
    smalls[1].wait()
    tail = [roll_buf[...]] if part == LANES else [roll_buf[...], jnp.zeros((1, LANES - part), jnp.float32)]
    packs[z, c.gain_rows :, :] = jnp.broadcast_to(
        jnp.concatenate(tail, axis=1), (8 - c.gain_rows, LANES)
    )
    m_buf[...] = jnp.full(m_buf.shape, LOW, jnp.float32)
    for ref in (l_buf, q_buf, p_buf):
        ref[...] = jnp.zeros(ref.shape, jnp.float32)
    smalls[0].wait()
    ids_all[g] = id_buf[...]
    load_x.wait()

    neighbours = jnp.where(has_right, 1, 0) + jnp.where(has_left, 1, 0)
    pl.semaphore_wait(barrier, len(peers) + neighbours)

    def piece(gi, q, zi):
        return x_buf.at[
            gi, pl.ds(pl.multiple_of(q * c.rows, c.rows), c.rows), pl.ds(pl.multiple_of(zi * c.dz, c.dz), c.dz)
        ]

    def w_block(fi, h, j):
        return w_full.at[
            pl.ds(pl.multiple_of(h * c.half_cols + j * c.chunk, c.chunk), c.chunk),
            pl.ds(pl.multiple_of(fi * c.kr, c.kr), c.kr),
        ]

    def y_tokens(n, act):
        for d in range(1, G):
            q = n - (G - d) * T

            @pl.when((q >= 0) & (q < T))
            def _(d=d, q=q):
                act(remote(piece(g, q, z), piece(g, q, z), y_send.at[d - 1], y_recv.at[G - d - 1, q], dev_g(group(d))))

    def y_weights(j, act):
        for d in range(1, G):
            gi = group(d)
            src = w_stage.at[gi, pl.ds(pl.multiple_of(j * c.chunk, c.chunk), c.chunk), :]
            act(remote(src, w_block(f, x, j), wy_send.at[d - 1], wy_recv.at[G - d - 1, j], dev_g(gi)))

    def hop_ends(s):
        return ((z - s >= 0, jnp.maximum(z - s, 0), has_right, right_dev, right_send, pack_right),
                (z + s < Z, jnp.minimum(z + s, Z - 1), has_left, left_dev, left_send, pack_left))

    def locate(n):
        return group(n // T), lax.rem(n, T), lax.rem(n, Z_RING)

    def hop_wait(n, s):
        gi, q, slot = locate(n)
        if s == 0:
            @pl.when(n >= T)
            def _():
                arrive(piece(gi, q, z), y_recv.at[n // T - 1, q])
            return
        for ok, zi, _, _, _, _ in hop_ends(s):
            @pl.when(ok)
            def _():
                arrive(piece(gi, q, zi), tok_recv.at[slot, zi])

    def hop_send(n, s, act):
        gi, q, slot = locate(n)
        for ok, zi, has, dev, sem, _ in hop_ends(s):
            @pl.when(ok & has)
            def _():
                act(remote(piece(gi, q, zi), piece(gi, q, zi), sem.at[zi], tok_recv.at[slot, zi], dev))

    def pack_wait(s):
        for ok, zi, _, _, _, _ in hop_ends(s):
            @pl.when(ok)
            def _():
                arrive(packs.at[zi], pack_recv.at[zi])

    def pack_hop(s, act):
        for ok, zi, has, dev, _, sem in hop_ends(s):
            @pl.when(ok & has)
            def _():
                act(remote(packs.at[zi], packs.at[zi], sem.at[zi], pack_recv.at[zi], dev))

    def core_pass(src, fi, h, j, act):
        gi = fi // 2
        act(remote(src, w_block(fi, h, j), core_send.at[gi, h], core_recv.at[j], partner))

    def x_weights(d, fi, j, act):
        for dx in range(1, DP):
            act(remote(w_block(fi, x, j), w_block(fi, x, j), wx_send.at[d - 1, dx - 1],
                       wx_recv.at[d - 1, DP - dx - 1, j], dev_x(lax.rem(x + dx, DP))))

    def ids_move(act):
        for d in range(1, G):
            act(remote(id_buf, ids_all.at[g], ids_send.at[d - 1], ids_recv.at[G - d - 1], dev_g(group(d))))

    def roll_move(act):
        for dx in range(DP):
            for df in range(F):
                if dx or df:
                    act(remote(row_buf, roll.at[me_resp], roll_send, roll_recv,
                               (lax.rem(x + dx, DP), lax.rem(f + df, F), z)))

    def stats_move(p, late, act):
        d, half = p // c.group_pairs, lax.rem(p, c.group_pairs)
        gi = group(d)
        for s in range(Z - 1, -1, -1):
            def go(s=s):
                act(remote(s_out.at[p], s_all.at[half * (G * Z) + g * Z + z], st_send.at[late], st_recv.at[late],
                           (x, gi * 2 + core, lax.rem(z + s, Z))))
            if s:
                go()
            else:
                pl.when(d > 0)(go)

    def normalize(n):
        gi, q, _ = locate(n)
        values = x_buf[gi, pl.ds(pl.multiple_of(q * c.rows, c.rows), c.rows), :].astype(jnp.float32)
        inv = lax.rsqrt(jnp.sum(values * values, axis=1, keepdims=True) / c.dim + norm_eps)
        there = pl.ds(pl.multiple_of(n * c.rows, c.rows), c.rows)
        for zi in range(Z):
            for r in range(c.gain_rows):
                here = slice(zi * c.dz + r * LANES, zi * c.dz + (r + 1) * LANES)
                scaled = values[:, here] * inv * packs[zi, r : r + 1, :]
                n_buf[there, here] = scaled.astype(jnp.bfloat16)

    def unit(p, k, halves=None, span_cols=None):
        n_cols = span_cols or c.unit_cols
        tokens = n_buf[pl.ds(pl.multiple_of(p * c.width, c.width), c.width), :]
        index = lax.broadcasted_iota(jnp.int32, (n_cols // 8, 8, 1), 0) * 8 + lax.broadcasted_iota(
            jnp.int32, (n_cols // 8, 8, 1), 1
        )
        for h in (range(DP) if halves is None else halves):
            off = h * c.half_cols + k * n_cols
            cols = pl.ds(pl.multiple_of(off, c.chunk), n_cols)
            logits = lax.dot_general(
                w_full[cols, :], tokens, (((1,), (1,)), ((), ())), preferred_element_type=jnp.float32
            ).reshape(n_cols // 8, 8, c.width)
            valid = c.vt - g * c.block_cols - off
            place = rel[p] - off
            p_buf[p] = p_buf[p] + jnp.sum(jnp.where(index == place[None], logits, 0.0), axis=0)
            if (G - 1) * c.block_cols + (h + 1) * c.half_cols > c.vt:
                logits = jnp.where(index < valid, logits, LOW)
            before = m_buf[p]
            top = jnp.maximum(before, jnp.max(logits, axis=0))
            scale = jnp.exp(before - top)
            e = jnp.exp(logits - top[None])
            m_buf[p] = top
            l_buf[p] = l_buf[p] * scale + jnp.sum(e, axis=0)
            q_buf[p] = q_buf[p] * (scale * scale) + jnp.sum(e * e, axis=0)

    def collect(p):
        m_p = m_buf[p]
        top = jnp.max(m_p, axis=0, keepdims=True)
        scale = jnp.exp(m_p - top)
        total = jnp.sum(l_buf[p] * scale, axis=0, keepdims=True)
        square = jnp.sum(q_buf[p] * (scale * scale), axis=0, keepdims=True)
        picked = jnp.sum(p_buf[p], axis=0, keepdims=True)
        s_out[p] = jnp.concatenate([top, total, square, picked], axis=0)

    def collect_send(p, late):
        p = jnp.int32(p)
        collect(p)
        stats_move(p, late, begin)

        @pl.when(p < c.group_pairs)
        def _():
            s_all[p * (G * Z) + g * Z + z] = s_out[p]

    pack_hop(0, begin)
    ids_move(begin)

    def wait_loads(stage):
        def act(own, size, copy, gi, h):
            if size and own != stage:
                copy().wait()
        weight_loads(act)

    def tick(i, seen):
        w_first, y_first, x_first, r_first, u_first = seen

        @pl.when(i == 0)
        def _():
            wait_loads(True)

        w_end = due(i, c.w_tick)

        @pl.when(i + LEAD < N)
        def _():
            y_tokens(i + LEAD, begin)

        @pl.loop(w_first, w_end)
        def _(j):
            y_weights(j, begin)

        for s in range(Z):
            q = i - s

            @pl.when((q >= 0) & (q < N))
            def _(s=s, q=q):
                if s:
                    @pl.when(q == 0)
                    def _():
                        pack_wait(s)
                        if s < Z - 1:
                            pack_hop(s, begin)
                hop_wait(q, s)
                if s < Z - 1:
                    hop_send(q, s, begin)

        @pl.when(i == 1)
        def _():
            wait_loads(False)

        for n in range(2):
            j = 2 * (i - 1) + n

            @pl.when((j >= 0) & (j < J))
            def _(j=j):
                for h in range(DP):
                    core_pass(w_block(f, h, j), f, h, j, begin)

        r_end = due(i, c.r_tick)

        @pl.loop(r_first, r_end)
        def _(j):
            arrive(w_full.at[pl.ds(0, G * DP * c.kr * c.chunk // c.dim), :], core_recv.at[j])

        y_end = due(i, c.y_tick)

        @pl.loop(y_first, y_end)
        def _(j):
            for d in range(1, G):
                gi = group(d)
                fi = gi * 2 + core
                arrive(w_block(fi, x, j), wy_recv.at[d - 1, j])
                x_weights(d, fi, j, begin)
                core_pass(w_block(fi, x, j), fi, x, j, begin)

        x_end = due(i, c.x_tick)

        @pl.loop(x_first, x_end)
        def _(j):
            for d in range(1, G):
                gi = group(d)
                fi = gi * 2 + core
                for dx in range(1, DP):
                    xi = lax.rem(x + dx, DP)
                    arrive(w_block(fi, xi, j), wx_recv.at[d - 1, dx - 1, j])
                    core_pass(w_block(fi, xi, j), fi, xi, j, begin)

        q = i - (Z - 1)

        @pl.when((q >= 0) & (q < N))
        def _():
            normalize(q)

        @pl.when(i == Z)
        def _():
            for zi in range(Z):
                row_buf[:, zi * part : (zi + 1) * part] = packs[zi, c.gain_rows : c.gain_rows + 1, :part]
            for d in range(1, G):
                arrive(ids_all.at[group(d)], ids_recv.at[d - 1])
            base = z * c.vt + g * c.block_cols
            for d in range(G):
                for half in range(c.group_pairs):
                    ids = ids_all[group(d), :, half * c.width : (half + 1) * c.width]
                    rel[d * c.group_pairs + half] = jnp.broadcast_to(ids - base, (8, c.width))

        u_end = lookup(i, c.counts)

        @pl.loop(u_first, u_end)
        def _(u):
            unit(lookup(u, [p for p, _ in c.order]), lookup(u, [k for _, k in c.order]))

        return w_end, y_end, x_end, r_end, u_end

    lax.fori_loop(0, c.ticks, tick, (jnp.int32(0),) * 5)
    roll_move(begin)
    pl.loop(0, c.pairs - 1)(lambda p: collect_send(p, 0))
    wide = 2 if c.blocks % 2 == 0 else 1

    for k in range(c.blocks // wide):
        for h in range(DP):
            unit(c.pairs - 1, k, (h,), wide * c.unit_cols)
    collect_send(c.pairs - 1, 1)

    for copy in smalls[3:]:
        copy.wait()
    def done(ref, sem):
        remote(ref, ref, sem, sem, partner).wait_send()

    def features(gi, zi):
        return x_buf.at[gi, :, pl.ds(pl.multiple_of(zi * c.dz, c.dz), c.dz)]

    stage = w_stage.at[0]
    for d in range(1, G):
        done(features(g, z), y_send.at[d - 1])
        done(stage, wy_send.at[d - 1])
        for dx in range(1, DP):
            done(stage, wx_send.at[d - 1, dx - 1])
    for gi in range(G):
        for h in range(DP):
            done(stage, core_send.at[gi, h])
    for zi in range(Z):
        for cond, sem in (((zi <= z) & has_right, right_send), ((zi >= z) & has_left, left_send)):
            @pl.when(cond)
            def _():
                done(x_buf.at[:, :, pl.ds(zi * c.dz, c.dz)], sem.at[zi])

    for s in range(Z - 1):
        pack_hop(s, sent)
    ids_move(sent)
    roll[me_resp] = row_buf[...]
    arrive(roll.at[pl.ds(0, c.resp - 1)], roll_recv)
    ref = jnp.zeros((1, c.tok), jnp.float32)
    row = row_in[...]
    for r in range(c.resp):
        ref = ref + jnp.where(row == r, roll[r], 0.0)
    position = lax.broadcasted_iota(jnp.int32, (1, c.tok), 1)
    live = jnp.where(position < len_in[...], 1.0, 0.0)
    old, adv = old_buf[...], adv_buf[...]

    early = c.group_pairs * (G * Z - 1) - Z
    arrive(s_all.at[pl.ds(0, early)], st_recv.at[0])
    arrive(s_all.at[pl.ds(0, Z)], st_recv.at[1])
    every = [(gi, zi) for gi in range(G) for zi in range(Z)]

    def stat(gi, zi, k):
        return jnp.concatenate([s_all[p * (G * Z) + gi * Z + zi, k : k + 1, :] for p in range(c.group_pairs)], axis=1)

    top = stat(0, 0, 0)
    for gi, zi in every[1:]:
        top = jnp.maximum(top, stat(gi, zi, 0))
    total = square = picked = jnp.zeros((1, c.tok), jnp.float32)
    for gi, zi in every:
        scale = jnp.exp(stat(gi, zi, 0) - top)
        total = total + stat(gi, zi, 1) * scale
        square = square + stat(gi, zi, 2) * (scale * scale)
        picked = picked + stat(gi, zi, 3)
    new_logp = picked - top - jnp.log(total)
    prob_square = square / (total * total)
    token_loss, kl_part, grad_part = token_terms(new_logp, old, adv, ref, live, prob_square)
    sums = [jnp.sum(v, axis=1, keepdims=True) for v in (live, token_loss, kl_part, grad_part)]
    t_out[...] = jnp.concatenate(
        [jnp.broadcast_to(v, (1, LANES)) for v in sums] + [jnp.zeros((4, LANES), jnp.float32)], axis=0
    )

    def totals_move(act):
        for dx in range(DP):
            for df in range(F):
                if dx or df:
                    act(remote(t_out, t_in.at[me_resp], tot_send, tot_recv,
                               (lax.rem(x + dx, DP), lax.rem(f + df, F), z)))

    totals_move(begin)
    t_in[me_resp] = t_out[...]
    out[0:1, :] = new_logp
    out[1:2, :] = token_loss
    out[3:8, :] = jnp.zeros((5, c.tok), jnp.float32)
    done(roll.at[pl.ds(0, c.resp - 1)], roll_send)
    done(s_all.at[pl.ds(0, early)], st_send.at[0])
    done(s_all.at[pl.ds(0, Z)], st_send.at[1])
    arrive(t_in.at[pl.ds(0, c.resp - 1)], tot_recv)
    totals = sum(t_in[r] for r in range(c.resp))
    count = totals[0:1]
    lane = lax.broadcasted_iota(jnp.int32, (1, LANES), 1)
    means = jnp.where(lane == 0, totals[1:2] / count,
                      jnp.where(lane == 1, totals[2:3] / count, jnp.sqrt(totals[3:4] / count)))
    out[2:3, :] = jnp.concatenate([means] * (c.tok // LANES), axis=1)
    done(t_in.at[pl.ds(0, c.resp - 1)], tot_send)


def split(src, logp, loss, summary):
    logp[...] = src[0:1, :]
    loss[...] = src[1:2, :]
    summary[...] = src[2:3, 0:3].reshape(3)


def shards(c_of, hidden, norm_gain, head_weight, token_ids, lengths, old_logp, advantages, rollout_logp, rollout_row):
    c = c_of(hidden.shape[0], hidden.shape[1], head_weight.shape[0], head_weight.shape[1])
    G, Z, DP, F, T, J = c.groups, c.tz, c.dp, c.fs, c.group_steps, c.chunks
    vmem = pl.BlockSpec(memory_space=pltpu.VMEM)
    hbm = pl.BlockSpec(memory_space=pl.ANY)
    dma = lambda *shape: pltpu.SemaphoreType.DMA(shape)
    one_sem = pltpu.SemaphoreType.DMA
    f32, i32, b16 = jnp.float32, jnp.int32, jnp.bfloat16
    one = lambda dtype, lead=(): pltpu.VMEM((*lead, 1, c.tok), dtype)
    lanes = lambda dtype: pltpu.VMEM((c.pairs, 8, c.width), dtype)
    out = pl.pallas_call(
        functools.partial(kernel, c),
        out_shape=jax.ShapeDtypeStruct((8, c.tok), f32),
        in_specs=[hbm] * 9,
        out_specs=vmem,
        scratch_shapes=[
            one(i32), pltpu.VMEM(rollout_logp.shape, f32), one(f32), one(f32),
            pltpu.VMEM(norm_gain.shape, b16), pltpu.VMEM((1, 1), i32), pltpu.VMEM((1, 1), i32),
            pltpu.VMEM((G, c.tok, c.dim), b16),
            pltpu.VMEM((c.pairs * c.width, c.dim), b16),
            pltpu.VMEM((G, c.half_cols, c.kr), b16),
            pltpu.VMEM((c.block_cols, c.dim), b16),
            pltpu.VMEM((Z, 8, LANES), f32),
            one(i32, (G,)),
            lanes(i32), lanes(f32), lanes(f32), lanes(f32), lanes(f32),
            one(f32), one(f32, (c.resp,)),
            pltpu.VMEM((c.pairs, 4, c.width), f32),
            pltpu.VMEM((c.group_pairs * G * Z, 4, c.width), f32),
            pltpu.VMEM((8, LANES), f32),
            pltpu.VMEM((c.resp, 8, LANES), f32),
            dma(7), one_sem, dma(G), dma(DP), dma(Z_RING, Z), dma(G - 1, T), dma(G - 1), dma(Z), dma(Z),
            dma(G - 1), dma(G - 1, J), dma(G - 1, DP - 1), dma(G - 1, DP - 1, J), dma(G, DP), dma(J),
            dma(G - 1), dma(G - 1), dma(Z), dma(Z), dma(Z), one_sem, one_sem,
            dma(2), dma(2), one_sem, one_sem,
        ],
        compiler_params=pltpu.CompilerParams(
            collective_id=0, has_side_effects=True, vmem_limit_bytes=64 * 1024 * 1024 - 65536
        ),
    )(hidden, norm_gain, head_weight.T, token_ids, rollout_logp, old_logp, advantages,
      lengths.reshape(1, 1), rollout_row.reshape(1, 1))
    row = lambda n: jax.ShapeDtypeStruct((1, c.tok), f32)
    return pl.pallas_call(
        split,
        out_shape=(row(0), row(1), jax.ShapeDtypeStruct((3,), f32)),
        in_specs=[vmem],
        out_specs=(vmem, vmem, vmem),
    )(out)


def solution(mesh):
    rows = ("dp", "fsdp")
    in_specs = (
        P(rows, "tensor"), P("tensor"), P("fsdp", "tensor"), P(rows, None), P(rows),
        P(rows, None), P(rows, None), P(rows, "tensor"), P(rows),
    )
    out_specs = (P(rows, None), P(rows, None), P())
    return jax.shard_map(
        functools.partial(shards, functools.partial(Config, mesh)),
        mesh=mesh, in_specs=in_specs, out_specs=out_specs, check_vma=False,
    )
```
